32 devices in a mesh: grp: 2 (over x), tp: 4 (over y, core), pp: 4 (over z).
Axes of the slice: x: 2, y: 2, z: 4, core: 2. Of those that a mesh axis runs over, the one named last changes fastest.
Arguments:
- tokens: bfloat16 [1024, 8192], P('grp', 'tp'), parts along dimension 0, may hold values from -12 to 12
- gain: bfloat16 [4, 8192], P('pp', 'tp'), may hold values from 0.099609375 to 1.8984375
- q_weight: bfloat16 [4, 8192, 4096], P('pp', None, 'tp'), may hold values from -0.5 to 0.5
- kv_weight: bfloat16 [4, 8192, 2048], P('pp', None, 'tp'), may hold values from -0.5 to 0.5
- out_weight: bfloat16 [4, 4096, 8192], P('pp', None, 'tp'), may hold values from -0.09375 to 0.09375
- page_table: int32 [4, 8, 128], P('pp'), may hold values from 0 to 1023, as said below
- segment_ids: int32 [1024], P('grp'), parts along dimension 0, may hold values from 0 to 2, never falling along the last dimension, each value on 1 to 256 neighbouring positions
Outputs:
- hidden: bfloat16 [1024, 8192], P(('grp', 'pp'), 'tp'), parts along dimension 0
- kv_cache: bfloat16 [4, 2048, 4, 256], P('pp', ('grp', 'tp')), parts along dimension 1
The draws below stay inside these ranges and needn't reach their ends.
There are 2 independent parts, one for each index of `grp`. The reference program is written for one: setup_inputs(seed, part) draws one part's arguments, and reference() takes and returns one part's arrays. A program takes and returns all parts, laid end to end along the dimension named above; an argument that names none is the same for every part. Nothing has to cross between parts.
Inputs may be any that keep to these rules, and one draw needn't show every extreme that they name: `page_table`: every entry of a layer's table is distinct and every one of the 1024 values occurs once. For each layer, head and micro-batch the 16 blocks form a run; in each run half of the devices receive exactly 8 pages and the others none, so each device receives exactly 256 pages of a layer.
All inputs are finite; a program needn't handle non-finite values.
Results may differ from the reference program's by a relative error of at most 0.017.
Values may be sent and summed in bfloat16 or wider, within the bound.
A program may use at most 128 MiB of HBM per device.

```python
import math
import jax
import jax.numpy as jnp
import numpy as np
from jax import lax

MODEL_WIDTH = 8192
QUERY_HEADS = 32
HEAD_SIZE = 128
KEY_VALUE_HEADS = 8
MICRO_BATCHES = 8
PAGE_TOKENS = 4
LAYER_COUNT = 4
PREFIX_TOKENS = 512
MB_BLOCKS = 16
PREFIX_BLOCKS = 128
MOST = 8
CACHE_PAGES = 256
N_TP = 4


def draw_tokens(key, part):
    first_key = jax.random.fold_in(key, 21)
    ramp_cols = 0.6 + 1.2 * jnp.arange(MODEL_WIDTH, dtype=jnp.float32) / MODEL_WIDTH
    rough = jax.random.normal(first_key, (PREFIX_TOKENS, MODEL_WIDTH), jnp.float32)
    return jnp.clip(rough * ramp_cols, -12.0, 12.0).astype(jnp.bfloat16)


def joint_weights(key):
    query_key = jax.random.fold_in(key, 11)
    key_value_random = jax.random.fold_in(key, 12)
    inverse_sqrt_width = math.sqrt(MODEL_WIDTH)
    key_value_rows = jax.random.normal(key_value_random, (LAYER_COUNT, MODEL_WIDTH, 2 * KEY_VALUE_HEADS * HEAD_SIZE), jnp.float32) / inverse_sqrt_width
    local_portion = jax.random.normal(query_key, (LAYER_COUNT, MODEL_WIDTH, QUERY_HEADS * HEAD_SIZE), jnp.float32) / inverse_sqrt_width
    query_matrix = local_portion
    return (jnp.clip(query_matrix, -0.5, 0.5), jnp.clip(key_value_rows, -0.5, 0.5))


def draw_q_weight(key, part):
    return joint_weights(key)[0].astype(jnp.bfloat16)


def draw_kv_weight(key, part):
    return joint_weights(key)[1].astype(jnp.bfloat16)


def draw_page_table(key, part):
    device_total = 2 * MB_BLOCKS // MOST
    half_count = device_total // 2
    running_total = KEY_VALUE_HEADS * MICRO_BATCHES
    pick_key = jax.random.fold_in(key, 31)
    shuffle_key = jax.random.fold_in(key, 32)
    slot_key = jax.random.fold_in(key, 33)
    device_scores = jax.random.randint(pick_key, (LAYER_COUNT, running_total // 2, device_total), 0, 1 << 20) * device_total + jnp.arange(device_total, dtype=jnp.int32)
    device_order = jnp.argsort(device_scores, axis=-1).astype(jnp.int32)
    chosen = jnp.stack([device_order[:, :, :half_count], device_order[:, :, half_count:]], axis=2)
    chosen = chosen.reshape(LAYER_COUNT, running_total, half_count)
    page_store = jnp.tile(chosen, (1, 1, MOST))
    mix_scores = jax.random.randint(shuffle_key, (LAYER_COUNT, running_total, MB_BLOCKS), 0, 1 << 20) * MB_BLOCKS + jnp.arange(MB_BLOCKS, dtype=jnp.int32)
    mixing_permutation = jnp.argsort(mix_scores, axis=-1).astype(jnp.int32)
    target_pages = jnp.take_along_axis(page_store, mixing_permutation, axis=-1).reshape(LAYER_COUNT, KEY_VALUE_HEADS * PREFIX_BLOCKS)
    onehot = (target_pages[:, :, None] == jnp.arange(device_total, dtype=jnp.int32)[None, None, :]).astype(jnp.int32)
    earlier = jnp.cumsum(onehot, axis=1) - onehot
    arrival = jnp.sum(earlier * onehot, axis=2)
    slot_scores = jax.random.randint(slot_key, (LAYER_COUNT, device_total, CACHE_PAGES), 0, 1 << 20) * CACHE_PAGES + jnp.arange(CACHE_PAGES, dtype=jnp.int32)
    slot_order = jnp.argsort(slot_scores, axis=-1).astype(jnp.int32).reshape(LAYER_COUNT, device_total * CACHE_PAGES)
    cache_page_index = jnp.take_along_axis(slot_order, target_pages * CACHE_PAGES + arrival, axis=1)
    return (target_pages * CACHE_PAGES + cache_page_index).reshape(LAYER_COUNT, KEY_VALUE_HEADS, PREFIX_BLOCKS).astype(jnp.int32)


def block_scale(rng, dims, shards, least, largest):
    def one(dim, parts):
        heights = jax.random.uniform(jax.random.fold_in(jax.random.fold_in(rng, 6), dim), (parts,), jnp.float32, least / len(shards), largest / len(shards))
        return jnp.repeat(jnp.exp(heights), dims[dim] // parts).reshape((-1,) + (1,) * (len(dims) - dim - 1))

    loudness = one(*shards[0])
    for cut in shards[1:]:
        loudness = loudness * one(*cut)
    return loudness


def profile(count, total, most, slope):
    portions = [(1 << 20) // math.isqrt(grade ** slope) + 1 for grade in range(2, count + 1)]
    rest, given = total - most - (count - 1), [1] * (count - 1)
    while rest > 0:
        free = [i for i in range(count - 1) if given[i] < most]
        mass, budget = sum([portions[i] for i in free]), rest
        for i in free:
            more = min(most - given[i], max(1, budget * portions[i] // mass), rest)
            given[i] = given[i] + more
            rest = rest - more
    return np.array([most] + given)


def ragged_sizes(rng, count, total, most, slope):
    if count == 2:
        one = jax.random.randint(rng, (), max(1, total - most), min(most, total - 1) + 1)
        return jnp.stack([one, total - one])
    tallies = jnp.asarray(profile(count, total, most, slope), jnp.int32)
    couples = (count - 1) // 2
    giver, taker = tallies[1:1 + 2 * couples:2], tallies[2:2 + 2 * couples:2]
    room = jnp.minimum(giver - 1, most - taker)
    moved = jax.random.randint(jax.random.fold_in(rng, 1), (couples,), 0, 1 << 20) % (room + 1)
    tallies = tallies.at[1:1 + 2 * couples:2].set(giver - moved).at[2:2 + 2 * couples:2].set(taker + moved)
    return tallies[jax.random.permutation(jax.random.fold_in(rng, 2), count)]


def normal_values(rng, shape, width, most, shards=(), held_as=jnp.bfloat16):
    values = jax.random.normal(rng, shape, jnp.float32) * width
    if len(shards) > 0:
        values = block_scale(rng, shape, shards, -0.22, 0.18) * values
    return jnp.clip(values, min=-most, max=most).astype(held_as)


def setup_inputs(seed: int = 0, part: int = 0) -> dict:
    splits = jax.random.split(jax.random.key(seed), 8)
    part_splits = jax.random.split(jax.random.fold_in(splits[7], part), 8)
    tokens = draw_tokens(jax.random.fold_in(jax.random.fold_in(splits[7], part), 71), part)
    gain = jnp.clip(1.0 + 0.18 * jax.random.normal(splits[1], (LAYER_COUNT, MODEL_WIDTH), jnp.float32), 0.099609375, 1.8984375).astype(jnp.bfloat16)
    q_weight = draw_q_weight(jax.random.fold_in(splits[7], 71), part)
    kv_weight = draw_kv_weight(jax.random.fold_in(splits[7], 71), part)
    out_weight = normal_values(splits[4], (LAYER_COUNT, QUERY_HEADS * HEAD_SIZE, MODEL_WIDTH), (QUERY_HEADS * HEAD_SIZE) ** -0.5, 0.09375, ((0, 4), (2, 4)))
    page_table = draw_page_table(jax.random.fold_in(splits[7], 71), part)
    segment_ids = jnp.searchsorted(jnp.cumsum(ragged_sizes(part_splits[6], 3, PREFIX_TOKENS, PREFIX_TOKENS // 2, 2)), jnp.arange(PREFIX_TOKENS), side="right").astype(jnp.int32)
    return {"tokens": tokens, "gain": gain, "q_weight": q_weight, "kv_weight": kv_weight, "out_weight": out_weight, "page_table": page_table, "segment_ids": segment_ids}


eps_norm = 1e-05

def reference(tokens, gain, q_weight, kv_weight, out_weight, page_table, segment_ids):
    query_group_width = QUERY_HEADS // KEY_VALUE_HEADS
    score_scale = 1.0 / math.sqrt(HEAD_SIZE)
    positions = jnp.arange(PREFIX_TOKENS, dtype=jnp.int32)
    allowed = (positions[None, :] <= positions[:, None]) & (segment_ids[None, :] == segment_ids[:, None])
    stream = tokens
    caches = []
    for layer_idx in range(LAYER_COUNT):
        widened = stream.astype(jnp.float32)
        mean_sq = lax.optimization_barrier(jnp.sum(widened * widened, axis=1, keepdims=True)) / MODEL_WIDTH
        normed = (widened * lax.rsqrt(mean_sq + eps_norm) * gain[layer_idx].astype(jnp.float32)).astype(jnp.bfloat16)
        query_matrix = jnp.dot(normed, q_weight[layer_idx], preferred_element_type=jnp.float32).astype(jnp.bfloat16)
        key_value_rows = jnp.dot(normed, kv_weight[layer_idx], preferred_element_type=jnp.float32).astype(jnp.bfloat16)
        key_value_heads = key_value_rows.reshape(PREFIX_TOKENS, KEY_VALUE_HEADS, 2, HEAD_SIZE).astype(jnp.float32)
        grouped_queries = query_matrix.reshape(PREFIX_TOKENS, KEY_VALUE_HEADS, query_group_width, HEAD_SIZE).astype(jnp.float32)
        scores = jnp.einsum('qgpd,kgd->gpqk', grouped_queries, key_value_heads[:, :, 0]) * score_scale
        scores = jnp.where(allowed[None, None], scores, -1e+30)
        row_max = lax.optimization_barrier(jnp.max(scores, axis=-1, keepdims=True))
        raised = jnp.exp(scores - row_max)
        weights = (raised / lax.optimization_barrier(jnp.sum(raised, axis=-1, keepdims=True))).astype(jnp.bfloat16)
        mixed_heads = jnp.einsum('gpqk,kgd->qgpd', weights.astype(jnp.float32), key_value_heads[:, :, 1])
        mixed_heads = mixed_heads.astype(jnp.bfloat16).reshape(PREFIX_TOKENS, QUERY_HEADS * HEAD_SIZE)
        update = jnp.dot(mixed_heads, out_weight[layer_idx], preferred_element_type=jnp.float32)
        stream = (widened + update).astype(jnp.bfloat16)
        page_contents = key_value_rows.reshape(PREFIX_BLOCKS, PAGE_TOKENS, KEY_VALUE_HEADS, 2 * HEAD_SIZE).transpose(2, 0, 1, 3).reshape(KEY_VALUE_HEADS * PREFIX_BLOCKS, PAGE_TOKENS, 2 * HEAD_SIZE)
        filled = jnp.zeros((N_TP * CACHE_PAGES, PAGE_TOKENS, 2 * HEAD_SIZE), jnp.bfloat16).at[page_table[layer_idx].reshape(-1)].set(page_contents)
        caches.append(filled)
    return (stream, jnp.stack(caches))
```

```python
import functools
import math

import jax
import jax.numpy as jnp
from jax import lax
from jax.experimental import pallas as pl
from jax.experimental.pallas import tpu as pltpu
from jax.sharding import PartitionSpec as P

MODEL_WIDTH = 8192
HEAD_SIZE = 128
KEY_VALUE_HEADS = 8
PAGE_TOKENS = 4


eps_norm = 1e-05


def partner_2(x, axis, apart):
    return lax.ppermute(x, axis, [(i, i ^ 1 << apart) for i in range(lax.axis_size(axis))])


def shifted(x, axis, by):
    peers = lax.axis_size(axis)
    pairs = [(i, i + by) for i in range(peers) if 0 <= i + by < peers]
    return lax.ppermute(x, axis, pairs)


def own_pages(kv_buffer, page_rows, tp_rank, tensor_parallel_width, cache_page_count):
    row_total = kv_buffer.shape[0]
    blocks = row_total // PAGE_TOKENS
    copies = max(1, tensor_parallel_width // KEY_VALUE_HEADS)
    gathered = lax.all_gather(kv_buffer, "tp", axis=0, tiled=False)[::copies]
    head_width = 2 * HEAD_SIZE
    held = kv_buffer.shape[1] // head_width
    pages = (
        gathered.reshape(KEY_VALUE_HEADS // held, blocks, PAGE_TOKENS, held, head_width)
        .transpose(0, 3, 1, 2, 4)
        .reshape(KEY_VALUE_HEADS * blocks, PAGE_TOKENS * head_width)
    )
    slots = tp_rank * cache_page_count + jnp.arange(cache_page_count, dtype=jnp.int32)
    onehot = (page_rows.reshape(-1)[None, :] == slots[:, None]).astype(jnp.bfloat16)
    picked = jnp.dot(onehot, pages, preferred_element_type=jnp.float32).astype(jnp.bfloat16)
    return picked.reshape(cache_page_count, PAGE_TOKENS, head_width)


def body(tokens, gain, q_weight, kv_weight, out_weight, page_table, segment_ids):
    tensor_parallel_width = lax.axis_size("tp")
    pp_size = lax.axis_size("pp")
    tp_rank = lax.axis_index("tp")
    section_idx = lax.axis_index("pp")
    w_query = q_weight[0]
    w_keyval = kv_weight[0]
    w_output = out_weight[0]
    page_rows = page_table[0]
    local_width = tokens.shape[1]
    row_total = tokens.shape[0]
    micro_batches = pp_size
    row_count = row_total // micro_batches
    head_dim = HEAD_SIZE
    kv_cols = w_keyval.shape[1]
    held_heads = max(1, kv_cols // (2 * head_dim))
    q_heads = w_query.shape[1] // head_dim
    per_kv = q_heads // held_heads
    cache_page_count = KEY_VALUE_HEADS * (row_total // PAGE_TOKENS) // tensor_parallel_width
    score_scale = 1.0 / math.sqrt(head_dim)
    step_count = micro_batches + pp_size - 1
    gain_all = lax.all_gather(gain, "tp", axis=1, tiled=True).astype(jnp.float32)

    def add_columns(block_cols):
        return (
            jnp.dot(block_cols, w_query, preferred_element_type=jnp.float32),
            jnp.dot(block_cols, w_keyval, preferred_element_type=jnp.float32),
        )

    def add_outputs(block_cols):
        return jnp.dot(block_cols, w_output, preferred_element_type=jnp.float32)

    def one_step(step_idx, state_tuple):
        received, kv_buffer, hidden = state_tuple
        micro_raw = step_idx - section_idx
        is_live = (micro_raw >= 0) & (micro_raw < micro_batches)
        micro_idx = jnp.clip(micro_raw, 0, micro_batches - 1)
        row_start = micro_idx * row_count
        first_rows = lax.dynamic_slice_in_dim(tokens, row_start, row_count, 0)
        current = jnp.where(section_idx == 0, first_rows, received)
        whole_rows = lax.all_gather(current, "tp", axis=1, tiled=True).astype(jnp.float32)
        mean_sq = jnp.sum(whole_rows * whole_rows, axis=1, keepdims=True) / MODEL_WIDTH
        normed = (whole_rows * lax.rsqrt(mean_sq + eps_norm) * gain_all).astype(jnp.bfloat16)
        query_sum, keyval_sum = add_columns(normed)
        query_matrix = query_sum.astype(jnp.bfloat16)
        kv_own = keyval_sum.astype(jnp.bfloat16)
        if tensor_parallel_width > KEY_VALUE_HEADS:
            partner = partner_2(kv_own, "tp", 0)
            first_half = tp_rank % 2 == 0
            head_pair = jnp.where(
                first_half,
                jnp.concatenate([kv_own, partner], axis=1),
                jnp.concatenate([partner, kv_own], axis=1),
            )
        else:
            head_pair = kv_own
        refreshed = lax.dynamic_update_slice_in_dim(kv_buffer, head_pair, row_start, 0)
        kv_buffer = jnp.where(is_live, refreshed, kv_buffer)
        key_count = row_count * min(step_idx + 1, micro_batches)
        key_pos = jnp.arange(key_count, dtype=jnp.int32)
        kv_view = kv_buffer[:key_count].reshape(key_count, held_heads, 2, head_dim)
        grouped_queries = query_matrix.reshape(row_count, held_heads, per_kv, head_dim)
        scores = (
            jnp.einsum(
                "qgpd,kgd->gpqk",
                grouped_queries,
                kv_view[:, :, 0],
                preferred_element_type=jnp.float32,
            )
            * score_scale
        )
        query_pos = row_start + jnp.arange(row_count, dtype=jnp.int32)
        seg_query = lax.dynamic_slice_in_dim(segment_ids, row_start, row_count, 0)
        allowed = (key_pos[None, :] <= query_pos[:, None]) & (
            segment_ids[None, :key_count] == seg_query[:, None]
        )
        scores = jnp.where(allowed[None, None], scores, -1e30)
        row_max = jnp.max(scores, axis=-1, keepdims=True)
        raised = jnp.exp(scores - row_max)
        weights = (raised / jnp.sum(raised, axis=-1, keepdims=True)).astype(jnp.bfloat16)
        attended = jnp.einsum(
            "gpqk,kgd->qgpd", weights, kv_view[:, :, 1], preferred_element_type=jnp.float32
        )
        attended = attended.astype(jnp.bfloat16).reshape(row_count, q_heads * head_dim)
        projected = add_outputs(lax.all_gather(attended, "tp", axis=1, tiled=True))
        produced = (current.astype(jnp.float32) + projected).astype(jnp.bfloat16)
        done = step_idx - (pp_size - 1)
        if done >= 0:
            share = produced
            if done < pp_size - 1:
                share = lax.ppermute(produced, "pp", [(pp_size - 1, done)])
            hidden = jnp.where(section_idx == done, share, hidden)
        handed = shifted(produced, "pp", 1) if step_idx < step_count - 1 else produced
        return (handed, kv_buffer, hidden)

    initial = (
        jnp.zeros((row_count, local_width), jnp.bfloat16),
        jnp.zeros((row_total, held_heads * 2 * head_dim), jnp.bfloat16),
        jnp.zeros((row_count, local_width), jnp.bfloat16),
    )
    finished = initial
    for step_idx in range(step_count):
        finished = one_step(step_idx, finished)
    hidden = finished[2]
    kv_cache = own_pages(
        finished[1], page_rows, tp_rank, tensor_parallel_width, cache_page_count
    )
    return (hidden, kv_cache[None])


MESH = pl.DeviceIdType.MESH
LANES = 128
STREAM_CHUNKS = 2


def section_kernel(
    rows_of_mb,
    micro_batches,
    pp_size,
    tokens_hbm,
    gain_ref,
    wq_hbm,
    wkv_hbm,
    wo_hbm,
    ids_ref,
    seg_row_ref,
    seg_col_ref,
    hidden_hbm,
    cache_hbm,
    wq,
    wkv,
    wo,
    stream,
    attended,
    keyval,
    gains,
    scaled,
    acc,
    proj,
    squares,
    landed,
    cache,
    wq_sem,
    wkv_sem,
    wo_sem,
    token_sem,
    gain_send,
    gain_recv,
    z_send,
    z_recv,
    y_send,
    y_recv,
    d_send,
    d_recv,
    r_send,
    r_recv,
    ay_send,
    ay_recv,
    ad_send,
    ad_recv,
    ar_send,
    ar_recv,
    k_send,
    k_recv,
    h_send,
    h_recv,
    out_sem,
):
    R, M, C = rows_of_mb, micro_batches, STREAM_CHUNKS
    width = stream.shape[2]
    model_width = 4 * width
    att_width = attended.shape[2]
    kv_width = keyval.shape[2]
    total_rows = stream.shape[1]
    q_width = wq.shape[1]
    chunk = width // C
    t = lax.axis_index("tp")
    sec = lax.axis_index("pp")
    last = pp_size - 1
    core = t % 2
    near = t + 1 - 2 * core
    far = (t + 2) % 4
    cross = (near + 2) % 4
    sources = (t, near, far, cross)
    score_scale = 1.0 / math.sqrt(HEAD_SIZE)
    per_section = M // pp_size

    def rows(i):
        return pl.ds(pl.multiple_of(i * R, R), R)

    def cols(c):
        return pl.ds(c * chunk, chunk)

    def remote(src, dst, send, recv, device):
        return pltpu.make_async_remote_copy(
            src_ref=src, dst_ref=dst, send_sem=send, recv_sem=recv, device_id=device, device_id_type=MESH
        )

    def wq_copy(s):
        k = pl.ds(pl.multiple_of(s * width, width), width)
        return pltpu.make_async_copy(wq_hbm.at[0, k], wq.at[k], wq_sem.at[s])

    def wkv_copy(s):
        k = pl.ds(pl.multiple_of(s * width, width), width)
        return pltpu.make_async_copy(wkv_hbm.at[0, k], wkv.at[k], wkv_sem.at[s])

    def wo_copy(s):
        a = pl.ds(pl.multiple_of(s * att_width, att_width), att_width)
        return pltpu.make_async_copy(wo_hbm.at[0, a], wo.at[a], wo_sem.at[s])

    def token_copy(i):
        return pltpu.make_async_copy(tokens_hbm.at[rows(i)], stream.at[t, rows(i)], token_sem.at[i])

    def y_copy(i, c):
        part = stream.at[t, rows(i), cols(c)]
        return remote(part, part, y_send.at[i, c], y_recv.at[i, c], {"tp": far})

    def d_copy(i, c):
        part = stream.at[t, rows(i), cols(c)]
        return remote(part, part, d_send.at[i, c], d_recv.at[i, c], {"tp": near})

    def r_copy(i, c):
        part = stream.at[far, rows(i), cols(c)]
        return remote(part, part, r_send.at[i, c], r_recv.at[i, c], {"tp": near})

    def z_copy(i, c):
        part = stream.at[t, rows(i), cols(c)]
        return remote(part, part, z_send.at[i, c], z_recv.at[i, c], {"pp": jnp.minimum(sec + 1, last)})

    def ay_copy(i):
        part = attended.at[t, rows(i)]
        return remote(part, part, ay_send.at[i], ay_recv.at[i], {"tp": far})

    def ad_copy(i):
        part = attended.at[t, rows(i)]
        return remote(part, part, ad_send.at[i], ad_recv.at[i], {"tp": near})

    def ar_copy(i):
        part = attended.at[far, rows(i)]
        return remote(part, part, ar_send.at[i], ar_recv.at[i], {"tp": near})

    def h_copy(i):
        return remote(
            stream.at[t, rows(i)],
            landed.at[rows(i % per_section)],
            h_send.at[i],
            h_recv.at[i % per_section],
            {"pp": i // per_section},
        )

    def k_copy(kind):
        which, to = ((t, far), (t, near), (far, near))[kind]
        return remote(keyval.at[which], keyval.at[which], k_send.at[kind], k_recv.at[kind], {"tp": to})

    def gain_copy(kind):
        return remote(gain_ref, gains.at[t], gain_send.at[kind], gain_recv.at[kind], {"tp": (near, far, cross)[kind]})

    @pl.when(sec == 0)
    def _():
        for i in range(M):
            token_copy(i).start()

    for s in sources:
        wq_copy(s).start()
        wkv_copy(s).start()
    for s in sources:
        wo_copy(s).start()

    barrier = pltpu.get_barrier_semaphore()
    for peer in (near, far, cross):
        pl.semaphore_signal(barrier, inc=1, device_id={"tp": peer}, device_id_type=MESH)
    for step in range(1, pp_size):
        pl.semaphore_signal(barrier, inc=1, device_id={"pp": (sec + step) % pp_size}, device_id_type=MESH)
    pl.semaphore_wait(barrier, 3 + pp_size - 1)

    for kind in range(3):
        gain_copy(kind).start()
    keyval[t] = jnp.zeros((total_rows, kv_width), jnp.bfloat16)
    gains[t] = gain_ref[...]

    def forward(i, c):
        @pl.when(sec == 0)
        def _():
            if c == 0:
                token_copy(i).wait()

        @pl.when(sec > 0)
        def _():
            z_copy(i, c).wait_recv()

        y_copy(i, c).start()
        d_copy(i, c).start()

    def take(i, s, k0, kn, first):
        x = stream[s, rows(i), pl.ds(k0, kn)].astype(jnp.float32)
        sq = x * x
        part = sq[:, :LANES]
        for j in range(1, kn // LANES):
            part = part + sq[:, j * LANES : (j + 1) * LANES]
        squares[...] = part if first else squares[...] + part
        g = gains[s, :, pl.ds(k0, kn)].astype(jnp.float32)
        scaled[:, :kn] = (x * g).astype(jnp.bfloat16)
        y = scaled[:, :kn]
        k = pl.ds(pl.multiple_of(s * width + k0, chunk), kn)
        for w, lo, hi in ((wq, 0, q_width), (wkv, q_width, q_width + kv_width)):
            add = jnp.dot(y, w[k, :], preferred_element_type=jnp.float32)
            acc[:, lo:hi] = add if first else acc[:, lo:hi] + add

    def project(i):
        def arrived(s):
            @pl.when(i == 0)
            def _():
                wq_copy(s).wait()
                wkv_copy(s).wait()

        arrived(t)
        take(i, t, 0, width, True)
        arrived(near)
        for c in range(C):
            d_copy(i, c).wait_recv()
        take(i, near, 0, width, False)
        for c in range(C):
            y_copy(i, c).wait_recv()
            r_copy(i, c).start()
            if c == 0:
                arrived(far)
            take(i, far, c * chunk, chunk, False)
        arrived(cross)
        for c in range(C):
            r_copy(i, c).wait_recv()
            take(i, cross, c * chunk, chunk, False)

    def attend(i):
        mean_sq = jnp.sum(squares[...], axis=1, keepdims=True) / model_width
        scale = lax.rsqrt(mean_sq + eps_norm)
        q = (acc[:, :q_width] * scale).astype(jnp.bfloat16)
        keyval[t, rows(i)] = (acc[:, q_width:] * scale).astype(jnp.bfloat16)
        q_pos = i * R + lax.broadcasted_iota(jnp.int32, (R, total_rows), 0)
        k_pos = lax.broadcasted_iota(jnp.int32, (R, total_rows), 1)
        kept = (k_pos <= q_pos) & (seg_row_ref[...] == seg_col_ref[rows(i)])
        bias = jnp.where(kept, 0.0, -1e30).astype(jnp.float32)
        held = kv_width // (2 * HEAD_SIZE)
        per_kv = q_width // HEAD_SIZE // held
        for g in range(held):
            at = g * 2 * HEAD_SIZE
            keys = keyval[t, :, at : at + HEAD_SIZE]
            values = keyval[t, :, at + HEAD_SIZE : at + 2 * HEAD_SIZE]
            heads = range(g * per_kv, (g + 1) * per_kv)
            qg = jnp.concatenate([q[:, j * HEAD_SIZE : (j + 1) * HEAD_SIZE] for j in heads], axis=0)
            s = lax.dot_general(qg, keys, (((1,), (1,)), ((), ())), preferred_element_type=jnp.float32)
            s = s.reshape(per_kv, R, total_rows) * score_scale + bias[None]
            s = s.reshape(per_kv * R, total_rows)
            raised = jnp.exp(s - jnp.max(s, axis=-1, keepdims=True))
            mass = jnp.sum(raised, axis=-1, keepdims=True)
            mixed = jnp.dot(raised.astype(jnp.bfloat16), values, preferred_element_type=jnp.float32) / mass
            mixed = mixed.astype(jnp.bfloat16)
            for n, j in enumerate(heads):
                attended[t, rows(i), j * HEAD_SIZE : (j + 1) * HEAD_SIZE] = mixed[n * R : (n + 1) * R]
        ay_copy(i).start()
        ad_copy(i).start()

    def out_rows(s):
        return pl.ds(pl.multiple_of(s * att_width, att_width), att_width)

    def outputs(i):
        def arrived(s):
            @pl.when(i == 0)
            def _():
                wo_copy(s).wait()

        arrived(t)
        proj[...] = jnp.dot(attended[t, rows(i)], wo[out_rows(t), :], preferred_element_type=jnp.float32)
        ad_copy(i).wait_recv()
        arrived(near)
        proj[...] += jnp.dot(attended[near, rows(i)], wo[out_rows(near), :], preferred_element_type=jnp.float32)
        ay_copy(i).wait_recv()
        ar_copy(i).start()
        arrived(far)
        proj[...] += jnp.dot(attended[far, rows(i)], wo[out_rows(far), :], preferred_element_type=jnp.float32)
        for c in range(C):
            y_copy(i, c).wait_send()
            d_copy(i, c).wait_send()
        ar_copy(i).wait_recv()
        arrived(cross)
        for c in range(C):
            add = jnp.dot(attended[cross, rows(i)], wo[out_rows(cross), cols(c)], preferred_element_type=jnp.float32)
            whole = stream[t, rows(i), cols(c)].astype(jnp.float32) + (proj[:, cols(c)] + add)
            stream[t, rows(i), cols(c)] = whole.astype(jnp.bfloat16)

            @pl.when(sec < last)
            def _():
                z_copy(i, c).start()

        @pl.when((sec == last) & (i // per_section < last))
        def _():
            h_copy(i).start()

    for c in range(C):
        forward(0, c)
    for kind in range(3):
        gain_copy(kind).wait_recv()

    def one(i, carry):
        project(i)
        attend(i)

        @pl.when(i + 1 < M)
        def _():
            for c in range(C):
                forward(i + 1, c)

        outputs(i)
        return carry

    lax.fori_loop(0, M, one, 0)

    k_copy(0).start()
    k_copy(1).start()

    @pl.when(sec < last)
    def _():
        for n in range(per_section):
            h_copy(n).wait_recv()
        done = pltpu.make_async_copy(landed, hidden_hbm, out_sem.at[0])
        done.start()
        done.wait()

    @pl.when(sec == last)
    def _():
        done = pltpu.make_async_copy(
            stream.at[t, pl.ds((M - per_section) * R, per_section * R)], hidden_hbm, out_sem.at[0]
        )
        done.start()
        done.wait()

    k_copy(0).wait_recv()
    k_copy(2).start()
    k_copy(1).wait_recv()
    k_copy(2).wait_recv()
    cache_rows = cache.shape[0]
    block = cache_rows // 4
    held = kv_width // (2 * HEAD_SIZE)

    def assemble(b, carry):
        start = pl.multiple_of(b * block, block)
        slot = t * cache_rows + start + lax.broadcasted_iota(jnp.int32, (block, total_rows), 0)
        total = jnp.zeros((block, 2 * HEAD_SIZE), jnp.float32)
        for s in range(4):
            for g in range(held):
                head = s * held + g
                onehot = jnp.where(ids_ref[head : head + 1, :] == slot, 1.0, 0.0).astype(jnp.bfloat16)
                pages = keyval[s, :, g * 2 * HEAD_SIZE : (g + 1) * 2 * HEAD_SIZE]
                total = total + jnp.dot(onehot, pages, preferred_element_type=jnp.float32)
        cache[pl.ds(start, block), :] = total.astype(jnp.bfloat16)
        return carry

    lax.fori_loop(0, 4, assemble, 0)
    stored = pltpu.make_async_copy(cache, cache_hbm, out_sem.at[1])
    stored.start()

    def drain(i, carry):
        for c in range(C):
            r_copy(i, c).wait_send()

            @pl.when(sec < last)
            def _():
                z_copy(i, c).wait_send()

        ay_copy(i).wait_send()
        ad_copy(i).wait_send()
        ar_copy(i).wait_send()

        @pl.when((sec == last) & (i // per_section < last))
        def _():
            h_copy(i).wait_send()

        return carry

    lax.fori_loop(0, M, drain, 0)
    for kind in range(3):
        k_copy(kind).wait_send()
        gain_copy(kind).wait_send()
    stored.wait()


def kernel_body(tokens, gain, q_weight, kv_weight, out_weight, page_table, segment_ids):
    pp_size = lax.axis_size("pp")
    total_rows, width = tokens.shape
    M = 2 * pp_size
    R = total_rows // M
    q_width, kv_width = q_weight.shape[2], kv_weight.shape[2]
    att_all = out_weight.shape[1]
    att_width = att_all // 4
    heads, blocks = page_table.shape[1:]
    cache_rows = heads * total_rows // 4
    token_in_page = jnp.arange(total_rows, dtype=jnp.int32) % PAGE_TOKENS
    ids = jnp.repeat(page_table[0], PAGE_TOKENS, axis=1) * PAGE_TOKENS + token_in_page[None, :]
    any_spec = pl.BlockSpec(memory_space=pl.ANY)
    vmem_spec = pl.BlockSpec(memory_space=pltpu.VMEM)
    dma = pltpu.SemaphoreType.DMA
    C = STREAM_CHUNKS
    bf16, f32 = jnp.bfloat16, jnp.float32
    hidden, cache = pl.pallas_call(
        functools.partial(section_kernel, R, M, pp_size),
        out_shape=(
            jax.ShapeDtypeStruct((total_rows // pp_size, width), bf16),
            jax.ShapeDtypeStruct((cache_rows, 2 * HEAD_SIZE), bf16),
        ),
        in_specs=[any_spec, vmem_spec, any_spec, any_spec, any_spec, vmem_spec, vmem_spec, vmem_spec],
        out_specs=(any_spec, any_spec),
        scratch_shapes=[
            pltpu.VMEM((4 * width, q_width), bf16),
            pltpu.VMEM((4 * width, kv_width), bf16),
            pltpu.VMEM((att_all, width), bf16),
            pltpu.VMEM((4, total_rows, width), bf16),
            pltpu.VMEM((4, total_rows, att_width), bf16),
            pltpu.VMEM((4, total_rows, kv_width), bf16),
            pltpu.VMEM((4, 1, width), bf16),
            pltpu.VMEM((R, width), bf16),
            pltpu.VMEM((R, q_width + kv_width), f32),
            pltpu.VMEM((R, width), f32),
            pltpu.VMEM((R, LANES), f32),
            pltpu.VMEM((total_rows // pp_size, width), bf16),
            pltpu.VMEM((cache_rows, 2 * HEAD_SIZE), bf16),
            dma((4,)),
            dma((4,)),
            dma((4,)),
            dma((M,)),
            dma((3,)),
            dma((3,)),
            dma((M, C)),
            dma((M, C)),
            dma((M, C)),
            dma((M, C)),
            dma((M, C)),
            dma((M, C)),
            dma((M, C)),
            dma((M, C)),
            dma((M,)),
            dma((M,)),
            dma((M,)),
            dma((M,)),
            dma((M,)),
            dma((M,)),
            dma((3,)),
            dma((3,)),
            dma((M,)),
            dma((M // pp_size,)),
            dma((2,)),
        ],
        compiler_params=pltpu.CompilerParams(
            collective_id=0, has_side_effects=True, vmem_limit_bytes=67043328
        ),
    )(
        tokens,
        gain,
        q_weight,
        kv_weight,
        out_weight,
        ids,
        segment_ids[None, :],
        segment_ids[:, None],
    )
    pages = cache.reshape(1, cache_rows // PAGE_TOKENS, PAGE_TOKENS, 2 * HEAD_SIZE)
    return hidden, pages


def chosen_body(tokens, gain, q_weight, kv_weight, out_weight, page_table, segment_ids):
    whole_heads = kv_weight.shape[2] % (2 * HEAD_SIZE) == 0
    rows_fit = tokens.shape[0] % (32 * lax.axis_size("pp")) == 0
    if lax.axis_size("tp") == 4 and whole_heads and rows_fit:
        return kernel_body(tokens, gain, q_weight, kv_weight, out_weight, page_table, segment_ids)
    return body(tokens, gain, q_weight, kv_weight, out_weight, page_table, segment_ids)


def solution(mesh):
    placed = (
        P("grp", "tp"),
        P("pp", "tp"),
        P("pp", None, "tp"),
        P("pp", None, "tp"),
        P("pp", None, "tp"),
        P("pp", None, None),
        P("grp"),
    )
    return jax.shard_map(
        chosen_body,
        mesh=mesh,
        in_specs=placed,
        out_specs=(P(("grp", "pp"), "tp"), P("pp", ("grp", "tp"), None, None)),
        check_vma=False,
    )
```

```python
import functools
import math

import jax
import jax.numpy as jnp
from jax import lax
from jax.experimental import pallas as pl
from jax.experimental.pallas import tpu as pltpu
from jax.sharding import PartitionSpec as P

MODEL_WIDTH = 8192
HEAD_SIZE = 128
KEY_VALUE_HEADS = 8
PAGE_TOKENS = 4


eps_norm = 1e-05


def partner_2(x, axis, apart):
    return lax.ppermute(x, axis, [(i, i ^ 1 << apart) for i in range(lax.axis_size(axis))])


def shifted(x, axis, by):
    peers = lax.axis_size(axis)
    pairs = [(i, i + by) for i in range(peers) if 0 <= i + by < peers]
    return lax.ppermute(x, axis, pairs)


def own_pages(kv_buffer, page_rows, tp_rank, tensor_parallel_width, cache_page_count):
    row_total = kv_buffer.shape[0]
    blocks = row_total // PAGE_TOKENS
    copies = max(1, tensor_parallel_width // KEY_VALUE_HEADS)
    gathered = lax.all_gather(kv_buffer, "tp", axis=0, tiled=False)[::copies]
    head_width = 2 * HEAD_SIZE
    held = kv_buffer.shape[1] // head_width
    pages = (
        gathered.reshape(KEY_VALUE_HEADS // held, blocks, PAGE_TOKENS, held, head_width)
        .transpose(0, 3, 1, 2, 4)
        .reshape(KEY_VALUE_HEADS * blocks, PAGE_TOKENS * head_width)
    )
    slots = tp_rank * cache_page_count + jnp.arange(cache_page_count, dtype=jnp.int32)
    onehot = (page_rows.reshape(-1)[None, :] == slots[:, None]).astype(jnp.bfloat16)
    picked = jnp.dot(onehot, pages, preferred_element_type=jnp.float32).astype(jnp.bfloat16)
    return picked.reshape(cache_page_count, PAGE_TOKENS, head_width)


def body(tokens, gain, q_weight, kv_weight, out_weight, page_table, segment_ids):
    tensor_parallel_width = lax.axis_size("tp")
    pp_size = lax.axis_size("pp")
    tp_rank = lax.axis_index("tp")
    section_idx = lax.axis_index("pp")
    w_query = q_weight[0]
    w_keyval = kv_weight[0]
    w_output = out_weight[0]
    page_rows = page_table[0]
    local_width = tokens.shape[1]
    row_total = tokens.shape[0]
    micro_batches = pp_size
    row_count = row_total // micro_batches
    head_dim = HEAD_SIZE
    kv_cols = w_keyval.shape[1]
    held_heads = max(1, kv_cols // (2 * head_dim))
    q_heads = w_query.shape[1] // head_dim
    per_kv = q_heads // held_heads
    cache_page_count = KEY_VALUE_HEADS * (row_total // PAGE_TOKENS) // tensor_parallel_width
    score_scale = 1.0 / math.sqrt(head_dim)
    step_count = micro_batches + pp_size - 1
    gain_all = lax.all_gather(gain, "tp", axis=1, tiled=True).astype(jnp.float32)

    def add_columns(block_cols):
        return (
            jnp.dot(block_cols, w_query, preferred_element_type=jnp.float32),
            jnp.dot(block_cols, w_keyval, preferred_element_type=jnp.float32),
        )

    def add_outputs(block_cols):
        return jnp.dot(block_cols, w_output, preferred_element_type=jnp.float32)

    def one_step(step_idx, state_tuple):
        received, kv_buffer, hidden = state_tuple
        micro_raw = step_idx - section_idx
        is_live = (micro_raw >= 0) & (micro_raw < micro_batches)
        micro_idx = jnp.clip(micro_raw, 0, micro_batches - 1)
        row_start = micro_idx * row_count
        first_rows = lax.dynamic_slice_in_dim(tokens, row_start, row_count, 0)
        current = jnp.where(section_idx == 0, first_rows, received)
        whole_rows = lax.all_gather(current, "tp", axis=1, tiled=True).astype(jnp.float32)
        mean_sq = jnp.sum(whole_rows * whole_rows, axis=1, keepdims=True) / MODEL_WIDTH
        normed = (whole_rows * lax.rsqrt(mean_sq + eps_norm) * gain_all).astype(jnp.bfloat16)
        query_sum, keyval_sum = add_columns(normed)
        query_matrix = query_sum.astype(jnp.bfloat16)
        kv_own = keyval_sum.astype(jnp.bfloat16)
        if tensor_parallel_width > KEY_VALUE_HEADS:
            partner = partner_2(kv_own, "tp", 0)
            first_half = tp_rank % 2 == 0
            head_pair = jnp.where(
                first_half,
                jnp.concatenate([kv_own, partner], axis=1),
                jnp.concatenate([partner, kv_own], axis=1),
            )
        else:
            head_pair = kv_own
        refreshed = lax.dynamic_update_slice_in_dim(kv_buffer, head_pair, row_start, 0)
        kv_buffer = jnp.where(is_live, refreshed, kv_buffer)
        key_count = row_count * min(step_idx + 1, micro_batches)
        key_pos = jnp.arange(key_count, dtype=jnp.int32)
        kv_view = kv_buffer[:key_count].reshape(key_count, held_heads, 2, head_dim)
        grouped_queries = query_matrix.reshape(row_count, held_heads, per_kv, head_dim)
        scores = (
            jnp.einsum(
                "qgpd,kgd->gpqk",
                grouped_queries,
                kv_view[:, :, 0],
                preferred_element_type=jnp.float32,
            )
            * score_scale
        )
        query_pos = row_start + jnp.arange(row_count, dtype=jnp.int32)
        seg_query = lax.dynamic_slice_in_dim(segment_ids, row_start, row_count, 0)
        allowed = (key_pos[None, :] <= query_pos[:, None]) & (
            segment_ids[None, :key_count] == seg_query[:, None]
        )
        scores = jnp.where(allowed[None, None], scores, -1e30)
        row_max = jnp.max(scores, axis=-1, keepdims=True)
        raised = jnp.exp(scores - row_max)
        weights = (raised / jnp.sum(raised, axis=-1, keepdims=True)).astype(jnp.bfloat16)
        attended = jnp.einsum(
            "gpqk,kgd->qgpd", weights, kv_view[:, :, 1], preferred_element_type=jnp.float32
        )
        attended = attended.astype(jnp.bfloat16).reshape(row_count, q_heads * head_dim)
        projected = add_outputs(lax.all_gather(attended, "tp", axis=1, tiled=True))
        produced = (current.astype(jnp.float32) + projected).astype(jnp.bfloat16)
        done = step_idx - (pp_size - 1)
        if done >= 0:
            share = produced
            if done < pp_size - 1:
                share = lax.ppermute(produced, "pp", [(pp_size - 1, done)])
            hidden = jnp.where(section_idx == done, share, hidden)
        handed = shifted(produced, "pp", 1) if step_idx < step_count - 1 else produced
        return (handed, kv_buffer, hidden)

    initial = (
        jnp.zeros((row_count, local_width), jnp.bfloat16),
        jnp.zeros((row_total, held_heads * 2 * head_dim), jnp.bfloat16),
        jnp.zeros((row_count, local_width), jnp.bfloat16),
    )
    finished = initial
    for step_idx in range(step_count):
        finished = one_step(step_idx, finished)
    hidden = finished[2]
    kv_cache = own_pages(
        finished[1], page_rows, tp_rank, tensor_parallel_width, cache_page_count
    )
    return (hidden, kv_cache[None])


MESH = pl.DeviceIdType.MESH
LANES = 128
STREAM_CHUNKS = 4


def section_kernel(
    rows_of_mb,
    micro_batches,
    pp_size,
    tokens_hbm,
    gain_ref,
    wq_hbm,
    wkv_hbm,
    wo_hbm,
    table_ref,
    seg_row_ref,
    hidden_hbm,
    cache_hbm,
    wq,
    wkv,
    wo,
    stream,
    attended,
    keyval,
    gains,
    acc,
    proj,
    squares,
    landed,
    cache,
    seg_col,
    ids,
    wq_sem,
    wkv_sem,
    wo_sem,
    token_sem,
    gain_send,
    gain_recv,
    z_send,
    z_recv,
    y_send,
    y_recv,
    d_send,
    d_recv,
    r_send,
    r_recv,
    ay_send,
    ay_recv,
    ad_send,
    ad_recv,
    ar_send,
    ar_recv,
    k_send,
    k_recv,
    h_send,
    h_recv,
    out_sem,
):
    R, M, C = rows_of_mb, micro_batches, STREAM_CHUNKS
    width = stream.shape[2]
    model_width = 4 * width
    att_width = attended.shape[2]
    kv_width = keyval.shape[2]
    total_rows = stream.shape[1]
    q_width = wq.shape[1]
    chunk = width // C
    t = lax.axis_index("tp")
    sec = lax.axis_index("pp")
    last = pp_size - 1
    core = t % 2
    near = t + 1 - 2 * core
    far = (t + 2) % 4
    cross = (near + 2) % 4
    sources = (t, near, far, cross)
    score_scale = 1.0 / math.sqrt(HEAD_SIZE)
    per_section = M // pp_size

    def rows(i):
        return pl.ds(pl.multiple_of(i * R, R), R)

    def cols(c):
        return pl.ds(c * chunk, chunk)

    def remote(src, dst, send, recv, device):
        return pltpu.make_async_remote_copy(
            src_ref=src, dst_ref=dst, send_sem=send, recv_sem=recv, device_id=device, device_id_type=MESH
        )

    def wq_copy(s):
        k = pl.ds(pl.multiple_of(s * width, width), width)
        return pltpu.make_async_copy(wq_hbm.at[0, k], wq.at[k], wq_sem.at[s])

    def wkv_copy(s):
        k = pl.ds(pl.multiple_of(s * width, width), width)
        return pltpu.make_async_copy(wkv_hbm.at[0, k], wkv.at[k], wkv_sem.at[s])

    def wo_copy(s):
        a = pl.ds(pl.multiple_of(s * att_width, att_width), att_width)
        return pltpu.make_async_copy(wo_hbm.at[0, a], wo.at[a], wo_sem.at[s])

    def token_copy(i):
        return pltpu.make_async_copy(tokens_hbm.at[rows(i)], stream.at[t, rows(i)], token_sem.at[i])

    def y_copy(i, c):
        part = stream.at[t, rows(i), cols(c)]
        return remote(part, part, y_send.at[i, c], y_recv.at[i, c], {"tp": far})

    def d_copy(i, c):
        part = stream.at[t, rows(i), cols(c)]
        return remote(part, part, d_send.at[i, c], d_recv.at[i, c], {"tp": near})

    def r_copy(i, c):
        part = stream.at[far, rows(i), cols(c)]
        return remote(part, part, r_send.at[i, c], r_recv.at[i, c], {"tp": near})

    def z_copy(i, c):
        part = stream.at[t, rows(i), cols(c)]
        return remote(part, part, z_send.at[i, c], z_recv.at[i, c], {"pp": jnp.minimum(sec + 1, last)})

    def ay_copy(i):
        part = attended.at[t, rows(i)]
        return remote(part, part, ay_send.at[i], ay_recv.at[i], {"tp": far})

    def ad_copy(i):
        part = attended.at[t, rows(i)]
        return remote(part, part, ad_send.at[i], ad_recv.at[i], {"tp": near})

    def ar_copy(i):
        part = attended.at[far, rows(i)]
        return remote(part, part, ar_send.at[i], ar_recv.at[i], {"tp": near})

    def h_copy(i):
        return remote(
            stream.at[t, rows(i)],
            landed.at[rows(i % per_section)],
            h_send.at[i],
            h_recv.at[i % per_section],
            {"pp": i // per_section},
        )

    def k_copy(kind, i):
        which, to = ((t, far), (t, near), (far, near))[kind]
        part = keyval.at[which, rows(i)]
        return remote(part, part, k_send.at[kind, i], k_recv.at[kind, i], {"tp": to})

    def gain_copy(kind):
        return remote(gain_ref, gains.at[t], gain_send.at[kind], gain_recv.at[kind], {"tp": (near, far, cross)[kind]})

    @pl.when(sec == 0)
    def _():
        for i in range(M):
            token_copy(i).start()

    for s in sources:
        wq_copy(s).start()
        wkv_copy(s).start()
    for s in sources:
        wo_copy(s).start()

    barrier = pltpu.get_barrier_semaphore()
    for peer in (near, far, cross):
        pl.semaphore_signal(barrier, inc=1, device_id={"tp": peer}, device_id_type=MESH)
    for step in range(1, pp_size):
        pl.semaphore_signal(barrier, inc=1, device_id={"pp": (sec + step) % pp_size}, device_id_type=MESH)

    for n in range(total_rows // LANES):
        across = jnp.broadcast_to(seg_row_ref[:, n * LANES : (n + 1) * LANES].astype(jnp.float32), (LANES, LANES))
        seg_col[n * LANES : (n + 1) * LANES, :] = across.T
    heads, blocks = table_ref.shape[1:]
    spread = lax.broadcasted_iota(jnp.int32, (blocks, total_rows), 1) // PAGE_TOKENS
    spread = jnp.where(spread == lax.broadcasted_iota(jnp.int32, (blocks, total_rows), 0), 1.0, 0.0).astype(jnp.bfloat16)
    table = table_ref[0]
    upper = jnp.dot((table // 256).astype(jnp.float32).astype(jnp.bfloat16), spread, preferred_element_type=jnp.float32)
    lower = jnp.dot((table % 256).astype(jnp.float32).astype(jnp.bfloat16), spread, preferred_element_type=jnp.float32)
    in_page = lax.broadcasted_iota(jnp.int32, (heads, total_rows), 1) % PAGE_TOKENS
    ids[...] = (upper * 256.0 + lower) * PAGE_TOKENS + in_page.astype(jnp.float32)
    keyval[t] = jnp.zeros((total_rows, kv_width), jnp.bfloat16)
    gains[t] = gain_ref[...]
    pl.semaphore_wait(barrier, 3 + pp_size - 1)

    def forward(i, c):
        @pl.when(sec == 0)
        def _():
            if c == 0:
                token_copy(i).wait()

        @pl.when(sec > 0)
        def _():
            z_copy(i, c).wait_recv()

        y_copy(i, c).start()
        d_copy(i, c).start()

    def relay(i, c):
        y_copy(i, c).wait_recv()
        r_copy(i, c).start()

    def take(i, s):
        x = stream[s, rows(i)]
        wide = x.astype(jnp.float32)
        sq = wide * wide
        part = sq[:, :LANES]
        for j in range(1, width // LANES):
            part = part + sq[:, j * LANES : (j + 1) * LANES]
        y = x * gains[s]
        k = pl.ds(pl.multiple_of(s * width, width), width)
        return (
            part,
            jnp.dot(y, wq[k, :], preferred_element_type=jnp.float32),
            jnp.dot(y, wkv[k, :], preferred_element_type=jnp.float32),
        )

    def near_part(i):
        a, b = take(i, t), take(i, near)
        squares[...] = a[0] + b[0]
        acc[:, :q_width] = a[1] + b[1]
        acc[:, q_width:] = a[2] + b[2]

    def far_part(i):
        a = take(i, far)
        squares[...] += a[0]
        acc[:, :q_width] += a[1]
        acc[:, q_width:] += a[2]

    def attend(i):
        a = take(i, cross)
        mean_sq = jnp.sum(squares[...] + a[0], axis=1, keepdims=True) / model_width
        scale = lax.rsqrt(mean_sq + eps_norm)
        q = ((acc[:, :q_width] + a[1]) * scale).astype(jnp.bfloat16)
        keyval[t, rows(i)] = ((acc[:, q_width:] + a[2]) * scale).astype(jnp.bfloat16)
        q_pos = i * R + lax.broadcasted_iota(jnp.int32, (R, total_rows), 0)
        k_pos = lax.broadcasted_iota(jnp.int32, (R, total_rows), 1)
        same = seg_row_ref[...].astype(jnp.float32) == seg_col[rows(i), 0:1]
        bias = jnp.where((k_pos <= q_pos) & same, 0.0, -1e30).astype(jnp.float32)
        held = kv_width // (2 * HEAD_SIZE)
        per_kv = q_width // HEAD_SIZE // held
        for g in range(held):
            at = g * 2 * HEAD_SIZE
            keys = keyval[t, :, at : at + HEAD_SIZE]
            values = keyval[t, :, at + HEAD_SIZE : at + 2 * HEAD_SIZE]
            heads = range(g * per_kv, (g + 1) * per_kv)
            qg = jnp.concatenate([q[:, j * HEAD_SIZE : (j + 1) * HEAD_SIZE] for j in heads], axis=0)
            s = lax.dot_general(qg, keys, (((1,), (1,)), ((), ())), preferred_element_type=jnp.float32)
            s = s.reshape(per_kv, R, total_rows) * score_scale + bias[None]
            s = s.reshape(per_kv * R, total_rows)
            raised = jnp.exp(s - jnp.max(s, axis=-1, keepdims=True))
            mass = jnp.sum(raised, axis=-1, keepdims=True)
            mixed = jnp.dot(raised.astype(jnp.bfloat16), values, preferred_element_type=jnp.float32) / mass
            mixed = mixed.astype(jnp.bfloat16)
            for n, j in enumerate(heads):
                attended[t, rows(i), j * HEAD_SIZE : (j + 1) * HEAD_SIZE] = mixed[n * R : (n + 1) * R]
        ay_copy(i).start()
        ad_copy(i).start()

        @pl.when(sec == last)
        def _():
            k_copy(0, i).start()
            k_copy(1, i).start()

    def out_rows(s):
        return pl.ds(pl.multiple_of(s * att_width, att_width), att_width)

    def from_att(i, s, at):
        return jnp.dot(attended[s, rows(i)], wo[out_rows(s), at], preferred_element_type=jnp.float32)

    def near_out(i):
        ad_copy(i).wait_recv()
        every = slice(None)
        proj[...] = from_att(i, t, every) + from_att(i, near, every)

    def relay_att(i):
        ay_copy(i).wait_recv()
        ar_copy(i).start()

    def far_out(i):
        for c in range(C):
            y_copy(i, c).wait_send()
            d_copy(i, c).wait_send()
        ar_copy(i).wait_recv()
        wide = 2 * chunk
        for n in range(C // 2):
            at = pl.ds(n * wide, wide)
            add = from_att(i, far, at) + from_att(i, cross, at)
            whole = stream[t, rows(i), at].astype(jnp.float32) + (proj[:, at] + add)
            stream[t, rows(i), at] = whole.astype(jnp.bfloat16)

            @pl.when(sec < last)
            def _():
                z_copy(i, 2 * n).start()
                z_copy(i, 2 * n + 1).start()

        @pl.when((sec == last) & (i // per_section < last))
        def _():
            h_copy(i).start()

    cache_rows = cache.shape[0]
    block = cache_rows // 4
    held = kv_width // (2 * HEAD_SIZE)
    half = total_rows // 2

    def assemble(n):
        at = slice(n * half, (n + 1) * half)

        def one_block(b, carry):
            start = pl.multiple_of(b * block, block)
            row = lax.broadcasted_iota(jnp.int32, (block, half), 0)
            row = (row + t * cache_rows + start).astype(jnp.float32)
            total = jnp.zeros((block, 2 * HEAD_SIZE), jnp.float32)
            for s in range(4):
                for g in range(held):
                    head = s * held + g
                    onehot = jnp.where(ids[head : head + 1, at] == row, 1.0, 0.0).astype(jnp.bfloat16)
                    pages = keyval[s, at, g * 2 * HEAD_SIZE : (g + 1) * 2 * HEAD_SIZE]
                    total = total + jnp.dot(onehot, pages, preferred_element_type=jnp.float32)
            if n == 1:
                total = total + cache[pl.ds(start, block), :].astype(jnp.float32)
            cache[pl.ds(start, block), :] = total.astype(jnp.bfloat16)
            return carry

        lax.fori_loop(0, 4, one_block, 0)

    def relay_pages(i):
        k_copy(0, i).wait_recv()
        k_copy(2, i).start()

    def pages_in(lo, hi):
        def one_mb(i, carry):
            k_copy(1, i).wait_recv()
            k_copy(2, i).wait_recv()
            return carry

        lax.fori_loop(lo, hi, one_mb, 0)

    for kind in range(3):
        gain_copy(kind).start()
    for c in range(C):
        forward(0, c)
    wq_copy(t).wait()
    wkv_copy(t).wait()
    wq_copy(near).wait()
    wkv_copy(near).wait()
    for kind in range(3):
        gain_copy(kind).wait_recv()
    for c in range(C):
        d_copy(0, c).wait_recv()
    near_part(0)
    for c in range(C):
        relay(0, c)
    first, final = sec == 0, sec == last
    middle = (sec > 0) & (sec < last)

    @pl.when(first | final)
    def _():
        for c in range(C // 2):
            forward(1, c)

    wq_copy(far).wait()
    wkv_copy(far).wait()
    far_part(0)
    wq_copy(cross).wait()
    wkv_copy(cross).wait()

    @pl.when(middle)
    def _():
        for c in range(C // 2):
            forward(1, c)

    for c in range(C // 2, C):
        forward(1, c)
    for c in range(C):
        r_copy(0, c).wait_recv()
    attend(0)
    for s in sources:
        wo_copy(s).wait()

    def one(i, carry):
        def ahead(where, *chunks):
            @pl.when((i + 2 < M) & where)
            def _():
                for c in chunks:
                    forward(i + 2, c)

        for c in range(C):
            d_copy(i + 1, c).wait_recv()
        near_part(i + 1)
        ahead(first, 0, 1)
        ahead(sec > 0, 0)
        near_out(i)
        ahead(middle, 1)
        ahead(final, 1, 2)
        for c in range(C):
            relay(i + 1, c)
        far_part(i + 1)
        ahead(sec < last, 2)
        ahead(final, 3)
        relay_att(i)
        ahead(first, 3)
        for c in range(C):
            r_copy(i + 1, c).wait_recv()
        attend(i + 1)
        ahead(middle, 3)

        @pl.when(sec == last)
        def _():
            relay_pages(i)

        far_out(i)
        return carry

    lax.fori_loop(0, M - 1, one, 0)
    near_out(M - 1)

    @pl.when(sec == last)
    def _():
        pages_in(0, M // 2)
        assemble(0)

    relay_att(M - 1)

    @pl.when(sec == last)
    def _():
        relay_pages(M - 1)

    far_out(M - 1)

    @pl.when(sec < last)
    def _():
        def send_pages(i, carry):
            k_copy(0, i).start()
            k_copy(1, i).start()
            return carry

        def pass_pages(i, carry):
            relay_pages(i)
            return carry

        lax.fori_loop(0, M, send_pages, 0)
        lax.fori_loop(0, M, pass_pages, 0)
        pages_in(0, M // 2)
        assemble(0)
        for n in range(per_section):
            h_copy(n).wait_recv()
        done = pltpu.make_async_copy(landed, hidden_hbm, out_sem.at[0])
        done.start()
        done.wait()

    mine = stream.at[t, pl.ds((M - per_section) * R, per_section * R)]

    @pl.when(sec == last)
    def _():
        pltpu.make_async_copy(mine, hidden_hbm, out_sem.at[0]).start()

    pages_in(M // 2, M)
    assemble(1)
    stored = pltpu.make_async_copy(cache, cache_hbm, out_sem.at[1])
    stored.start()

    def drain(i, carry):
        for c in range(C):
            r_copy(i, c).wait_send()

            @pl.when(sec < last)
            def _():
                z_copy(i, c).wait_send()

        ay_copy(i).wait_send()
        ad_copy(i).wait_send()
        ar_copy(i).wait_send()
        for kind in range(3):
            k_copy(kind, i).wait_send()

        @pl.when((sec == last) & (i // per_section < last))
        def _():
            h_copy(i).wait_send()

        return carry

    lax.fori_loop(0, M, drain, 0)
    for kind in range(3):
        gain_copy(kind).wait_send()

    @pl.when(sec == last)
    def _():
        pltpu.make_async_copy(mine, hidden_hbm, out_sem.at[0]).wait()

    stored.wait()


def kernel_body(tokens, gain, q_weight, kv_weight, out_weight, page_table, segment_ids):
    pp_size = lax.axis_size("pp")
    total_rows, width = tokens.shape
    M = 2 * pp_size
    R = total_rows // M
    q_width, kv_width = q_weight.shape[2], kv_weight.shape[2]
    att_all = out_weight.shape[1]
    att_width = att_all // 4
    heads = page_table.shape[1]
    cache_rows = heads * total_rows // 4
    any_spec = pl.BlockSpec(memory_space=pl.ANY)
    vmem_spec = pl.BlockSpec(memory_space=pltpu.VMEM)
    dma = pltpu.SemaphoreType.DMA
    C = STREAM_CHUNKS
    bf16, f32 = jnp.bfloat16, jnp.float32
    hidden, cache = pl.pallas_call(
        functools.partial(section_kernel, R, M, pp_size),
        out_shape=(
            jax.ShapeDtypeStruct((total_rows // pp_size, width), bf16),
            jax.ShapeDtypeStruct((cache_rows, 2 * HEAD_SIZE), bf16),
        ),
        in_specs=[any_spec, vmem_spec, any_spec, any_spec, any_spec, vmem_spec, vmem_spec],
        out_specs=(any_spec, any_spec),
        scratch_shapes=[
            pltpu.VMEM((4 * width, q_width), bf16),
            pltpu.VMEM((4 * width, kv_width), bf16),
            pltpu.VMEM((att_all, width), bf16),
            pltpu.VMEM((4, total_rows, width), bf16),
            pltpu.VMEM((4, total_rows, att_width), bf16),
            pltpu.VMEM((4, total_rows, kv_width), bf16),
            pltpu.VMEM((4, 1, width), bf16),
            pltpu.VMEM((R, q_width + kv_width), f32),
            pltpu.VMEM((R, width), f32),
            pltpu.VMEM((R, LANES), f32),
            pltpu.VMEM((total_rows // pp_size, width), bf16),
            pltpu.VMEM((cache_rows, 2 * HEAD_SIZE), bf16),
            pltpu.VMEM((total_rows, LANES), f32),
            pltpu.VMEM((heads, total_rows), f32),
            dma((4,)),
            dma((4,)),
            dma((4,)),
            dma((M,)),
            dma((3,)),
            dma((3,)),
            dma((M, C)),
            dma((M, C)),
            dma((M, C)),
            dma((M, C)),
            dma((M, C)),
            dma((M, C)),
            dma((M, C)),
            dma((M, C)),
            dma((M,)),
            dma((M,)),
            dma((M,)),
            dma((M,)),
            dma((M,)),
            dma((M,)),
            dma((3, M)),
            dma((3, M)),
            dma((M,)),
            dma((M // pp_size,)),
            dma((2,)),
        ],
        compiler_params=pltpu.CompilerParams(
            collective_id=0, has_side_effects=True, vmem_limit_bytes=67043328
        ),
    )(
        tokens,
        gain,
        q_weight,
        kv_weight,
        out_weight,
        page_table,
        segment_ids[None, :],
    )
    pages = cache.reshape(1, cache_rows // PAGE_TOKENS, PAGE_TOKENS, 2 * HEAD_SIZE)
    return hidden, pages


def chosen_body(tokens, gain, q_weight, kv_weight, out_weight, page_table, segment_ids):
    whole_heads = kv_weight.shape[2] % (2 * HEAD_SIZE) == 0
    rows_fit = tokens.shape[0] % (32 * lax.axis_size("pp")) == 0
    if lax.axis_size("tp") == 4 and whole_heads and rows_fit:
        return kernel_body(tokens, gain, q_weight, kv_weight, out_weight, page_table, segment_ids)
    return body(tokens, gain, q_weight, kv_weight, out_weight, page_table, segment_ids)


def solution(mesh):
    placed = (
        P("grp", "tp"),
        P("pp", "tp"),
        P("pp", None, "tp"),
        P("pp", None, "tp"),
        P("pp", None, "tp"),
        P("pp", None, None),
        P("grp"),
    )
    return jax.shard_map(
        chosen_body,
        mesh=mesh,
        in_specs=placed,
        out_specs=(P(("grp", "pp"), "tp"), P("pp", ("grp", "tp"), None, None)),
        check_vma=False,
    )
```

```python
import functools
import math

import jax
import jax.numpy as jnp
from jax import lax
from jax.experimental import pallas as pl
from jax.experimental.pallas import tpu as pltpu
from jax.sharding import PartitionSpec as P

MODEL_WIDTH = 8192
HEAD_SIZE = 128
KEY_VALUE_HEADS = 8
PAGE_TOKENS = 4


eps_norm = 1e-05


def partner_2(x, axis, apart):
    return lax.ppermute(x, axis, [(i, i ^ 1 << apart) for i in range(lax.axis_size(axis))])


def shifted(x, axis, by):
    peers = lax.axis_size(axis)
    pairs = [(i, i + by) for i in range(peers) if 0 <= i + by < peers]
    return lax.ppermute(x, axis, pairs)


def own_pages(kv_buffer, page_rows, tp_rank, tensor_parallel_width, cache_page_count):
    row_total = kv_buffer.shape[0]
    blocks = row_total // PAGE_TOKENS
    copies = max(1, tensor_parallel_width // KEY_VALUE_HEADS)
    gathered = lax.all_gather(kv_buffer, "tp", axis=0, tiled=False)[::copies]
    head_width = 2 * HEAD_SIZE
    held = kv_buffer.shape[1] // head_width
    pages = (
        gathered.reshape(KEY_VALUE_HEADS // held, blocks, PAGE_TOKENS, held, head_width)
        .transpose(0, 3, 1, 2, 4)
        .reshape(KEY_VALUE_HEADS * blocks, PAGE_TOKENS * head_width)
    )
    slots = tp_rank * cache_page_count + jnp.arange(cache_page_count, dtype=jnp.int32)
    onehot = (page_rows.reshape(-1)[None, :] == slots[:, None]).astype(jnp.bfloat16)
    picked = jnp.dot(onehot, pages, preferred_element_type=jnp.float32).astype(jnp.bfloat16)
    return picked.reshape(cache_page_count, PAGE_TOKENS, head_width)


def body(tokens, gain, q_weight, kv_weight, out_weight, page_table, segment_ids):
    tensor_parallel_width = lax.axis_size("tp")
    pp_size = lax.axis_size("pp")
    tp_rank = lax.axis_index("tp")
    section_idx = lax.axis_index("pp")
    w_query = q_weight[0]
    w_keyval = kv_weight[0]
    w_output = out_weight[0]
    page_rows = page_table[0]
    local_width = tokens.shape[1]
    row_total = tokens.shape[0]
    micro_batches = pp_size
    row_count = row_total // micro_batches
    head_dim = HEAD_SIZE
    kv_cols = w_keyval.shape[1]
    held_heads = max(1, kv_cols // (2 * head_dim))
    q_heads = w_query.shape[1] // head_dim
    per_kv = q_heads // held_heads
    cache_page_count = KEY_VALUE_HEADS * (row_total // PAGE_TOKENS) // tensor_parallel_width
    score_scale = 1.0 / math.sqrt(head_dim)
    step_count = micro_batches + pp_size - 1
    gain_all = lax.all_gather(gain, "tp", axis=1, tiled=True).astype(jnp.float32)

    def add_columns(block_cols):
        return (
            jnp.dot(block_cols, w_query, preferred_element_type=jnp.float32),
            jnp.dot(block_cols, w_keyval, preferred_element_type=jnp.float32),
        )

    def add_outputs(block_cols):
        return jnp.dot(block_cols, w_output, preferred_element_type=jnp.float32)

    def one_step(step_idx, state_tuple):
        received, kv_buffer, hidden = state_tuple
        micro_raw = step_idx - section_idx
        is_live = (micro_raw >= 0) & (micro_raw < micro_batches)
        micro_idx = jnp.clip(micro_raw, 0, micro_batches - 1)
        row_start = micro_idx * row_count
        first_rows = lax.dynamic_slice_in_dim(tokens, row_start, row_count, 0)
        current = jnp.where(section_idx == 0, first_rows, received)
        whole_rows = lax.all_gather(current, "tp", axis=1, tiled=True).astype(jnp.float32)
        mean_sq = jnp.sum(whole_rows * whole_rows, axis=1, keepdims=True) / MODEL_WIDTH
        normed = (whole_rows * lax.rsqrt(mean_sq + eps_norm) * gain_all).astype(jnp.bfloat16)
        query_sum, keyval_sum = add_columns(normed)
        query_matrix = query_sum.astype(jnp.bfloat16)
        kv_own = keyval_sum.astype(jnp.bfloat16)
        if tensor_parallel_width > KEY_VALUE_HEADS:
            partner = partner_2(kv_own, "tp", 0)
            first_half = tp_rank % 2 == 0
            head_pair = jnp.where(
                first_half,
                jnp.concatenate([kv_own, partner], axis=1),
                jnp.concatenate([partner, kv_own], axis=1),
            )
        else:
            head_pair = kv_own
        refreshed = lax.dynamic_update_slice_in_dim(kv_buffer, head_pair, row_start, 0)
        kv_buffer = jnp.where(is_live, refreshed, kv_buffer)
        key_count = row_count * min(step_idx + 1, micro_batches)
        key_pos = jnp.arange(key_count, dtype=jnp.int32)
        kv_view = kv_buffer[:key_count].reshape(key_count, held_heads, 2, head_dim)
        grouped_queries = query_matrix.reshape(row_count, held_heads, per_kv, head_dim)
        scores = (
            jnp.einsum(
                "qgpd,kgd->gpqk",
                grouped_queries,
                kv_view[:, :, 0],
                preferred_element_type=jnp.float32,
            )
            * score_scale
        )
        query_pos = row_start + jnp.arange(row_count, dtype=jnp.int32)
        seg_query = lax.dynamic_slice_in_dim(segment_ids, row_start, row_count, 0)
        allowed = (key_pos[None, :] <= query_pos[:, None]) & (
            segment_ids[None, :key_count] == seg_query[:, None]
        )
        scores = jnp.where(allowed[None, None], scores, -1e30)
        row_max = jnp.max(scores, axis=-1, keepdims=True)
        raised = jnp.exp(scores - row_max)
        weights = (raised / jnp.sum(raised, axis=-1, keepdims=True)).astype(jnp.bfloat16)
        attended = jnp.einsum(
            "gpqk,kgd->qgpd", weights, kv_view[:, :, 1], preferred_element_type=jnp.float32
        )
        attended = attended.astype(jnp.bfloat16).reshape(row_count, q_heads * head_dim)
        projected = add_outputs(lax.all_gather(attended, "tp", axis=1, tiled=True))
        produced = (current.astype(jnp.float32) + projected).astype(jnp.bfloat16)
        done = step_idx - (pp_size - 1)
        if done >= 0:
            share = produced
            if done < pp_size - 1:
                share = lax.ppermute(produced, "pp", [(pp_size - 1, done)])
            hidden = jnp.where(section_idx == done, share, hidden)
        handed = shifted(produced, "pp", 1) if step_idx < step_count - 1 else produced
        return (handed, kv_buffer, hidden)

    initial = (
        jnp.zeros((row_count, local_width), jnp.bfloat16),
        jnp.zeros((row_total, held_heads * 2 * head_dim), jnp.bfloat16),
        jnp.zeros((row_count, local_width), jnp.bfloat16),
    )
    finished = initial
    for step_idx in range(step_count):
        finished = one_step(step_idx, finished)
    hidden = finished[2]
    kv_cache = own_pages(
        finished[1], page_rows, tp_rank, tensor_parallel_width, cache_page_count
    )
    return (hidden, kv_cache[None])


MESH = pl.DeviceIdType.MESH
LANES = 128
STREAM_CHUNKS = 4
MATMUL_ROWS = 128


def section_kernel(
    rows_of_mb,
    micro_batches,
    pp_size,
    tokens_hbm,
    gain_ref,
    wq_hbm,
    wkv_hbm,
    wo_hbm,
    table_ref,
    seg_row_ref,
    hidden_hbm,
    cache_hbm,
    wq,
    wkv,
    wo,
    stream,
    attended,
    keyval,
    gains,
    acc,
    proj,
    squares,
    landed,
    cache,
    seg_col,
    ids,
    wq_sem,
    wkv_sem,
    wo_sem,
    token_sem,
    gain_send,
    gain_recv,
    z_send,
    z_recv,
    y_send,
    y_recv,
    d_send,
    d_recv,
    r_send,
    r_recv,
    ay_send,
    ay_recv,
    ad_send,
    ad_recv,
    ar_send,
    ar_recv,
    k_send,
    k_recv,
    h_send,
    h_recv,
    out_sem,
):
    R, M, C = rows_of_mb, micro_batches, STREAM_CHUNKS
    width = stream.shape[2]
    model_width = 4 * width
    att_width = attended.shape[2]
    kv_width = keyval.shape[2]
    total_rows = stream.shape[1]
    q_width = wq.shape[1]
    chunk = width // C
    t = lax.axis_index("tp")
    sec = lax.axis_index("pp")
    last = pp_size - 1
    core = t % 2
    near = t + 1 - 2 * core
    far = (t + 2) % 4
    cross = (near + 2) % 4
    sources = (t, near, far, cross)
    score_scale = 1.0 / math.sqrt(HEAD_SIZE)
    per_section = M // pp_size

    def rows(i):
        return pl.ds(pl.multiple_of(i * R, R), R)

    def cols(c):
        return pl.ds(c * chunk, chunk)

    def remote(src, dst, send, recv, device):
        return pltpu.make_async_remote_copy(
            src_ref=src, dst_ref=dst, send_sem=send, recv_sem=recv, device_id=device, device_id_type=MESH
        )

    def wq_copy(s):
        k = pl.ds(pl.multiple_of(s * width, width), width)
        return pltpu.make_async_copy(wq_hbm.at[0, k], wq.at[k], wq_sem.at[s])

    def wkv_copy(s):
        k = pl.ds(pl.multiple_of(s * width, width), width)
        return pltpu.make_async_copy(wkv_hbm.at[0, k], wkv.at[k], wkv_sem.at[s])

    def wo_copy(s):
        a = pl.ds(pl.multiple_of(s * att_width, att_width), att_width)
        return pltpu.make_async_copy(wo_hbm.at[0, a], wo.at[a], wo_sem.at[s])

    def token_copy(i):
        return pltpu.make_async_copy(tokens_hbm.at[rows(i)], stream.at[t, rows(i)], token_sem.at[i])

    def y_copy(i, c):
        part = stream.at[t, rows(i), cols(c)]
        return remote(part, part, y_send.at[i, c], y_recv.at[i, c], {"tp": far})

    def d_copy(i, c):
        part = stream.at[t, rows(i), cols(c)]
        return remote(part, part, d_send.at[i, c], d_recv.at[i, c], {"tp": near})

    def r_copy(i, c):
        part = stream.at[far, rows(i), cols(c)]
        return remote(part, part, r_send.at[i, c], r_recv.at[i, c], {"tp": near})

    def z_copy(i, c):
        part = stream.at[t, rows(i), cols(c)]
        return remote(part, part, z_send.at[i, c], z_recv.at[i, c], {"pp": jnp.minimum(sec + 1, last)})

    def ay_copy(i):
        part = attended.at[t, rows(i)]
        return remote(part, part, ay_send.at[i], ay_recv.at[i], {"tp": far})

    def ad_copy(i):
        part = attended.at[t, rows(i)]
        return remote(part, part, ad_send.at[i], ad_recv.at[i], {"tp": near})

    def ar_copy(i):
        part = attended.at[far, rows(i)]
        return remote(part, part, ar_send.at[i], ar_recv.at[i], {"tp": near})

    def h_copy(i):
        return remote(
            stream.at[t, rows(i)],
            landed.at[rows(i % per_section)],
            h_send.at[i],
            h_recv.at[i % per_section],
            {"pp": i // per_section},
        )

    def k_copy(kind, i):
        which, to = ((t, far), (t, near), (far, near))[kind]
        part = keyval.at[which, rows(i)]
        return remote(part, part, k_send.at[kind, i], k_recv.at[kind, i], {"tp": to})

    def gain_copy(kind):
        return remote(gain_ref, gains.at[t], gain_send.at[kind], gain_recv.at[kind], {"tp": (near, far, cross)[kind]})

    @pl.when(sec == 0)
    def _():
        for i in range(M):
            token_copy(i).start()

    for s in sources:
        wq_copy(s).start()
        wkv_copy(s).start()
    for s in sources:
        wo_copy(s).start()

    barrier = pltpu.get_barrier_semaphore()
    for peer in (near, far, cross):
        pl.semaphore_signal(barrier, inc=1, device_id={"tp": peer}, device_id_type=MESH)
    for step in range(1, pp_size):
        pl.semaphore_signal(barrier, inc=1, device_id={"pp": (sec + step) % pp_size}, device_id_type=MESH)

    for n in range(total_rows // LANES):
        across = jnp.broadcast_to(seg_row_ref[:, n * LANES : (n + 1) * LANES].astype(jnp.float32), (LANES, LANES))
        seg_col[n * LANES : (n + 1) * LANES, :] = across.T
    heads, blocks = table_ref.shape[1:]
    spread = lax.broadcasted_iota(jnp.int32, (blocks, total_rows), 1) // PAGE_TOKENS
    spread = jnp.where(spread == lax.broadcasted_iota(jnp.int32, (blocks, total_rows), 0), 1.0, 0.0).astype(jnp.bfloat16)
    table = table_ref[0]
    upper = jnp.dot((table // 256).astype(jnp.float32).astype(jnp.bfloat16), spread, preferred_element_type=jnp.float32)
    lower = jnp.dot((table % 256).astype(jnp.float32).astype(jnp.bfloat16), spread, preferred_element_type=jnp.float32)
    in_page = lax.broadcasted_iota(jnp.int32, (heads, total_rows), 1) % PAGE_TOKENS
    ids[...] = (upper * 256.0 + lower) * PAGE_TOKENS + in_page.astype(jnp.float32)
    keyval[t] = jnp.zeros((total_rows, kv_width), jnp.bfloat16)
    gains[t] = gain_ref[...]
    pl.semaphore_wait(barrier, 3 + pp_size - 1)

    def forward(i, c):
        @pl.when(sec == 0)
        def _():
            if c == 0:
                token_copy(i).wait()

        @pl.when(sec > 0)
        def _():
            z_copy(i, c).wait_recv()

        y_copy(i, c).start()
        d_copy(i, c).start()

    def relay(i, c):
        y_copy(i, c).wait_recv()
        r_copy(i, c).start()

    def product(x, w):
        n = x.shape[0]
        if 2 * n <= MATMUL_ROWS:
            x = jnp.concatenate([x, x], axis=0)
        return jnp.dot(x, w, preferred_element_type=jnp.float32)[:n]

    def take(i, s):
        x = stream[s, rows(i)]
        wide = x.astype(jnp.float32)
        sq = wide * wide
        part = sq[:, :LANES]
        for j in range(1, width // LANES):
            part = part + sq[:, j * LANES : (j + 1) * LANES]
        y = x * gains[s]
        k = pl.ds(pl.multiple_of(s * width, width), width)
        return part, product(y, wq[k, :]), product(y, wkv[k, :])

    def near_part(i):
        a, b = take(i, t), take(i, near)
        squares[...] = a[0] + b[0]
        acc[:, :q_width] = a[1] + b[1]
        acc[:, q_width:] = a[2] + b[2]

    def far_part(i):
        a = take(i, far)
        squares[...] += a[0]
        acc[:, :q_width] += a[1]
        acc[:, q_width:] += a[2]

    def attend(i):
        a = take(i, cross)
        mean_sq = jnp.sum(squares[...] + a[0], axis=1, keepdims=True) / model_width
        scale = lax.rsqrt(mean_sq + eps_norm)
        q = ((acc[:, :q_width] + a[1]) * scale).astype(jnp.bfloat16)
        keyval[t, rows(i)] = ((acc[:, q_width:] + a[2]) * scale).astype(jnp.bfloat16)
        q_pos = i * R + lax.broadcasted_iota(jnp.int32, (R, total_rows), 0)
        k_pos = lax.broadcasted_iota(jnp.int32, (R, total_rows), 1)
        same = seg_row_ref[...].astype(jnp.float32) == seg_col[rows(i), 0:1]
        bias = jnp.where((k_pos <= q_pos) & same, 0.0, -1e30).astype(jnp.float32)
        held = kv_width // (2 * HEAD_SIZE)
        per_kv = q_width // HEAD_SIZE // held
        for g in range(held):
            at = g * 2 * HEAD_SIZE
            keys = keyval[t, :, at : at + HEAD_SIZE]
            values = keyval[t, :, at + HEAD_SIZE : at + 2 * HEAD_SIZE]
            heads = range(g * per_kv, (g + 1) * per_kv)
            qg = jnp.concatenate([q[:, j * HEAD_SIZE : (j + 1) * HEAD_SIZE] for j in heads], axis=0)
            s = lax.dot_general(qg, keys, (((1,), (1,)), ((), ())), preferred_element_type=jnp.float32)
            s = s.reshape(per_kv, R, total_rows) * score_scale + bias[None]
            s = s.reshape(per_kv * R, total_rows)
            raised = jnp.exp(s - jnp.max(s, axis=-1, keepdims=True))
            mass = jnp.sum(raised, axis=-1, keepdims=True)
            mixed = jnp.dot(raised.astype(jnp.bfloat16), values, preferred_element_type=jnp.float32) / mass
            mixed = mixed.astype(jnp.bfloat16)
            for n, j in enumerate(heads):
                attended[t, rows(i), j * HEAD_SIZE : (j + 1) * HEAD_SIZE] = mixed[n * R : (n + 1) * R]
        ay_copy(i).start()
        ad_copy(i).start()

        @pl.when(sec == last)
        def _():
            k_copy(0, i).start()
            k_copy(1, i).start()

    def out_rows(s):
        return pl.ds(pl.multiple_of(s * att_width, att_width), att_width)

    def from_att(i, s, at):
        return product(attended[s, rows(i)], wo[out_rows(s), at])

    def near_out(i):
        ad_copy(i).wait_recv()
        every = slice(None)
        proj[...] = from_att(i, t, every) + from_att(i, near, every)

    def relay_att(i):
        ay_copy(i).wait_recv()
        ar_copy(i).start()

    def far_out(i):
        for c in range(C):
            y_copy(i, c).wait_send()
            d_copy(i, c).wait_send()
        ar_copy(i).wait_recv()
        wide = 2 * chunk
        for n in range(C // 2):
            at = pl.ds(n * wide, wide)
            add = from_att(i, far, at) + from_att(i, cross, at)
            whole = stream[t, rows(i), at].astype(jnp.float32) + (proj[:, at] + add)
            stream[t, rows(i), at] = whole.astype(jnp.bfloat16)

            @pl.when(sec < last)
            def _():
                z_copy(i, 2 * n).start()
                z_copy(i, 2 * n + 1).start()

        @pl.when((sec == last) & (i // per_section < last))
        def _():
            h_copy(i).start()

    cache_rows = cache.shape[0]
    block = cache_rows // 4
    held = kv_width // (2 * HEAD_SIZE)
    half = total_rows // 2

    def assemble(n):
        at = slice(n * half, (n + 1) * half)

        def one_block(b, carry):
            start = pl.multiple_of(b * block, block)
            row = lax.broadcasted_iota(jnp.int32, (block, half), 0)
            row = (row + t * cache_rows + start).astype(jnp.float32)
            total = jnp.zeros((block, 2 * HEAD_SIZE), jnp.float32)
            for s in range(4):
                for g in range(held):
                    head = s * held + g
                    onehot = jnp.where(ids[head : head + 1, at] == row, 1.0, 0.0).astype(jnp.bfloat16)
                    pages = keyval[s, at, g * 2 * HEAD_SIZE : (g + 1) * 2 * HEAD_SIZE]
                    total = total + jnp.dot(onehot, pages, preferred_element_type=jnp.float32)
            if n == 1:
                total = total + cache[pl.ds(start, block), :].astype(jnp.float32)
            cache[pl.ds(start, block), :] = total.astype(jnp.bfloat16)
            return carry

        lax.fori_loop(0, 4, one_block, 0)

    def relay_pages(i):
        k_copy(0, i).wait_recv()
        k_copy(2, i).start()

    def pages_in(lo, hi):
        def one_mb(i, carry):
            k_copy(1, i).wait_recv()
            k_copy(2, i).wait_recv()
            return carry

        lax.fori_loop(lo, hi, one_mb, 0)

    for kind in range(3):
        gain_copy(kind).start()
    for c in range(C):
        forward(0, c)
    wq_copy(t).wait()
    wkv_copy(t).wait()
    wq_copy(near).wait()
    wkv_copy(near).wait()
    for kind in range(3):
        gain_copy(kind).wait_recv()
    for c in range(C):
        d_copy(0, c).wait_recv()
    near_part(0)
    for c in range(C):
        relay(0, c)
    first, final = sec == 0, sec == last
    middle = (sec > 0) & (sec < last)

    @pl.when(first | final)
    def _():
        for c in range(C // 2):
            forward(1, c)

    wq_copy(far).wait()
    wkv_copy(far).wait()
    far_part(0)
    wq_copy(cross).wait()
    wkv_copy(cross).wait()

    @pl.when(middle)
    def _():
        for c in range(C // 2):
            forward(1, c)

    for c in range(C // 2, C):
        forward(1, c)
    for c in range(C):
        r_copy(0, c).wait_recv()
    attend(0)
    for s in sources:
        wo_copy(s).wait()

    def one(i, carry):
        def ahead(where, *chunks):
            @pl.when((i + 2 < M) & where)
            def _():
                for c in chunks:
                    forward(i + 2, c)

        for c in range(C):
            d_copy(i + 1, c).wait_recv()
        near_part(i + 1)
        ahead(first, 0, 1)
        ahead(sec > 0, 0)
        near_out(i)
        ahead(middle, 1)
        ahead(final, 1, 2)
        for c in range(C):
            relay(i + 1, c)
        far_part(i + 1)
        ahead(sec < last, 2)
        ahead(final, 3)
        relay_att(i)
        ahead(first, 3)
        for c in range(C):
            r_copy(i + 1, c).wait_recv()
        attend(i + 1)
        ahead(middle, 3)

        @pl.when(sec == last)
        def _():
            relay_pages(i)

        far_out(i)
        return carry

    lax.fori_loop(0, M - 1, one, 0)
    near_out(M - 1)

    @pl.when(sec == last)
    def _():
        pages_in(0, M // 2)
        assemble(0)

    relay_att(M - 1)

    @pl.when(sec == last)
    def _():
        relay_pages(M - 1)

    far_out(M - 1)

    @pl.when(sec < last)
    def _():
        def send_pages(i, carry):
            k_copy(0, i).start()
            k_copy(1, i).start()
            return carry

        def pass_pages(i, carry):
            relay_pages(i)
            return carry

        lax.fori_loop(0, M, send_pages, 0)
        lax.fori_loop(0, M, pass_pages, 0)
        pages_in(0, M // 2)
        assemble(0)
        for n in range(per_section):
            h_copy(n).wait_recv()
        done = pltpu.make_async_copy(landed, hidden_hbm, out_sem.at[0])
        done.start()
        done.wait()

    mine = stream.at[t, pl.ds((M - per_section) * R, per_section * R)]

    @pl.when(sec == last)
    def _():
        pltpu.make_async_copy(mine, hidden_hbm, out_sem.at[0]).start()

    pages_in(M // 2, M)
    assemble(1)
    stored = pltpu.make_async_copy(cache, cache_hbm, out_sem.at[1])
    stored.start()

    def drain(i, carry):
        for c in range(C):
            r_copy(i, c).wait_send()

            @pl.when(sec < last)
            def _():
                z_copy(i, c).wait_send()

        ay_copy(i).wait_send()
        ad_copy(i).wait_send()
        ar_copy(i).wait_send()
        for kind in range(3):
            k_copy(kind, i).wait_send()

        @pl.when((sec == last) & (i // per_section < last))
        def _():
            h_copy(i).wait_send()

        return carry

    lax.fori_loop(0, M, drain, 0)
    for kind in range(3):
        gain_copy(kind).wait_send()

    @pl.when(sec == last)
    def _():
        pltpu.make_async_copy(mine, hidden_hbm, out_sem.at[0]).wait()

    stored.wait()


def kernel_body(tokens, gain, q_weight, kv_weight, out_weight, page_table, segment_ids):
    pp_size = lax.axis_size("pp")
    total_rows, width = tokens.shape
    M = 2 * pp_size
    R = total_rows // M
    q_width, kv_width = q_weight.shape[2], kv_weight.shape[2]
    att_all = out_weight.shape[1]
    att_width = att_all // 4
    heads = page_table.shape[1]
    cache_rows = heads * total_rows // 4
    any_spec = pl.BlockSpec(memory_space=pl.ANY)
    vmem_spec = pl.BlockSpec(memory_space=pltpu.VMEM)
    dma = pltpu.SemaphoreType.DMA
    C = STREAM_CHUNKS
    bf16, f32 = jnp.bfloat16, jnp.float32
    hidden, cache = pl.pallas_call(
        functools.partial(section_kernel, R, M, pp_size),
        out_shape=(
            jax.ShapeDtypeStruct((total_rows // pp_size, width), bf16),
            jax.ShapeDtypeStruct((cache_rows, 2 * HEAD_SIZE), bf16),
        ),
        in_specs=[any_spec, vmem_spec, any_spec, any_spec, any_spec, vmem_spec, vmem_spec],
        out_specs=(any_spec, any_spec),
        scratch_shapes=[
            pltpu.VMEM((4 * width, q_width), bf16),
            pltpu.VMEM((4 * width, kv_width), bf16),
            pltpu.VMEM((att_all, width), bf16),
            pltpu.VMEM((4, total_rows, width), bf16),
            pltpu.VMEM((4, total_rows, att_width), bf16),
            pltpu.VMEM((4, total_rows, kv_width), bf16),
            pltpu.VMEM((4, 1, width), bf16),
            pltpu.VMEM((R, q_width + kv_width), f32),
            pltpu.VMEM((R, width), f32),
            pltpu.VMEM((R, LANES), f32),
            pltpu.VMEM((total_rows // pp_size, width), bf16),
            pltpu.VMEM((cache_rows, 2 * HEAD_SIZE), bf16),
            pltpu.VMEM((total_rows, LANES), f32),
            pltpu.VMEM((heads, total_rows), f32),
            dma((4,)),
            dma((4,)),
            dma((4,)),
            dma((M,)),
            dma((3,)),
            dma((3,)),
            dma((M, C)),
            dma((M, C)),
            dma((M, C)),
            dma((M, C)),
            dma((M, C)),
            dma((M, C)),
            dma((M, C)),
            dma((M, C)),
            dma((M,)),
            dma((M,)),
            dma((M,)),
            dma((M,)),
            dma((M,)),
            dma((M,)),
            dma((3, M)),
            dma((3, M)),
            dma((M,)),
            dma((M // pp_size,)),
            dma((2,)),
        ],
        compiler_params=pltpu.CompilerParams(
            collective_id=0, has_side_effects=True, vmem_limit_bytes=67043328
        ),
    )(
        tokens,
        gain,
        q_weight,
        kv_weight,
        out_weight,
        page_table,
        segment_ids[None, :],
    )
    pages = cache.reshape(1, cache_rows // PAGE_TOKENS, PAGE_TOKENS, 2 * HEAD_SIZE)
    return hidden, pages


def chosen_body(tokens, gain, q_weight, kv_weight, out_weight, page_table, segment_ids):
    whole_heads = kv_weight.shape[2] % (2 * HEAD_SIZE) == 0
    rows_fit = tokens.shape[0] % (32 * lax.axis_size("pp")) == 0
    if lax.axis_size("tp") == 4 and whole_heads and rows_fit:
        return kernel_body(tokens, gain, q_weight, kv_weight, out_weight, page_table, segment_ids)
    return body(tokens, gain, q_weight, kv_weight, out_weight, page_table, segment_ids)


def solution(mesh):
    placed = (
        P("grp", "tp"),
        P("pp", "tp"),
        P("pp", None, "tp"),
        P("pp", None, "tp"),
        P("pp", None, "tp"),
        P("pp", None, None),
        P("grp"),
    )
    return jax.shard_map(
        chosen_body,
        mesh=mesh,
        in_specs=placed,
        out_specs=(P(("grp", "pp"), "tp"), P("pp", ("grp", "tp"), None, None)),
        check_vma=False,
    )
```

```python
import functools
import math

import jax
import jax.numpy as jnp
from jax import lax
from jax.experimental import pallas as pl
from jax.experimental.pallas import tpu as pltpu
from jax.sharding import PartitionSpec as P

MODEL_WIDTH = 8192
HEAD_SIZE = 128
KEY_VALUE_HEADS = 8
PAGE_TOKENS = 4


eps_norm = 1e-05


def partner_2(x, axis, apart):
    return lax.ppermute(x, axis, [(i, i ^ 1 << apart) for i in range(lax.axis_size(axis))])


def shifted(x, axis, by):
    peers = lax.axis_size(axis)
    pairs = [(i, i + by) for i in range(peers) if 0 <= i + by < peers]
    return lax.ppermute(x, axis, pairs)


def own_pages(kv_buffer, page_rows, tp_rank, tensor_parallel_width, cache_page_count):
    row_total = kv_buffer.shape[0]
    blocks = row_total // PAGE_TOKENS
    copies = max(1, tensor_parallel_width // KEY_VALUE_HEADS)
    gathered = lax.all_gather(kv_buffer, "tp", axis=0, tiled=False)[::copies]
    head_width = 2 * HEAD_SIZE
    held = kv_buffer.shape[1] // head_width
    pages = (
        gathered.reshape(KEY_VALUE_HEADS // held, blocks, PAGE_TOKENS, held, head_width)
        .transpose(0, 3, 1, 2, 4)
        .reshape(KEY_VALUE_HEADS * blocks, PAGE_TOKENS * head_width)
    )
    slots = tp_rank * cache_page_count + jnp.arange(cache_page_count, dtype=jnp.int32)
    onehot = (page_rows.reshape(-1)[None, :] == slots[:, None]).astype(jnp.bfloat16)
    picked = jnp.dot(onehot, pages, preferred_element_type=jnp.float32).astype(jnp.bfloat16)
    return picked.reshape(cache_page_count, PAGE_TOKENS, head_width)


def body(tokens, gain, q_weight, kv_weight, out_weight, page_table, segment_ids):
    tensor_parallel_width = lax.axis_size("tp")
    pp_size = lax.axis_size("pp")
    tp_rank = lax.axis_index("tp")
    section_idx = lax.axis_index("pp")
    w_query = q_weight[0]
    w_keyval = kv_weight[0]
    w_output = out_weight[0]
    page_rows = page_table[0]
    local_width = tokens.shape[1]
    row_total = tokens.shape[0]
    micro_batches = pp_size
    row_count = row_total // micro_batches
    head_dim = HEAD_SIZE
    kv_cols = w_keyval.shape[1]
    held_heads = max(1, kv_cols // (2 * head_dim))
    q_heads = w_query.shape[1] // head_dim
    per_kv = q_heads // held_heads
    cache_page_count = KEY_VALUE_HEADS * (row_total // PAGE_TOKENS) // tensor_parallel_width
    score_scale = 1.0 / math.sqrt(head_dim)
    step_count = micro_batches + pp_size - 1
    gain_all = lax.all_gather(gain, "tp", axis=1, tiled=True).astype(jnp.float32)

    def add_columns(block_cols):
        return (
            jnp.dot(block_cols, w_query, preferred_element_type=jnp.float32),
            jnp.dot(block_cols, w_keyval, preferred_element_type=jnp.float32),
        )

    def add_outputs(block_cols):
        return jnp.dot(block_cols, w_output, preferred_element_type=jnp.float32)

    def one_step(step_idx, state_tuple):
        received, kv_buffer, hidden = state_tuple
        micro_raw = step_idx - section_idx
        is_live = (micro_raw >= 0) & (micro_raw < micro_batches)
        micro_idx = jnp.clip(micro_raw, 0, micro_batches - 1)
        row_start = micro_idx * row_count
        first_rows = lax.dynamic_slice_in_dim(tokens, row_start, row_count, 0)
        current = jnp.where(section_idx == 0, first_rows, received)
        whole_rows = lax.all_gather(current, "tp", axis=1, tiled=True).astype(jnp.float32)
        mean_sq = jnp.sum(whole_rows * whole_rows, axis=1, keepdims=True) / MODEL_WIDTH
        normed = (whole_rows * lax.rsqrt(mean_sq + eps_norm) * gain_all).astype(jnp.bfloat16)
        query_sum, keyval_sum = add_columns(normed)
        query_matrix = query_sum.astype(jnp.bfloat16)
        kv_own = keyval_sum.astype(jnp.bfloat16)
        if tensor_parallel_width > KEY_VALUE_HEADS:
            partner = partner_2(kv_own, "tp", 0)
            first_half = tp_rank % 2 == 0
            head_pair = jnp.where(
                first_half,
                jnp.concatenate([kv_own, partner], axis=1),
                jnp.concatenate([partner, kv_own], axis=1),
            )
        else:
            head_pair = kv_own
        refreshed = lax.dynamic_update_slice_in_dim(kv_buffer, head_pair, row_start, 0)
        kv_buffer = jnp.where(is_live, refreshed, kv_buffer)
        key_count = row_count * min(step_idx + 1, micro_batches)
        key_pos = jnp.arange(key_count, dtype=jnp.int32)
        kv_view = kv_buffer[:key_count].reshape(key_count, held_heads, 2, head_dim)
        grouped_queries = query_matrix.reshape(row_count, held_heads, per_kv, head_dim)
        scores = (
            jnp.einsum(
                "qgpd,kgd->gpqk",
                grouped_queries,
                kv_view[:, :, 0],
                preferred_element_type=jnp.float32,
            )
            * score_scale
        )
        query_pos = row_start + jnp.arange(row_count, dtype=jnp.int32)
        seg_query = lax.dynamic_slice_in_dim(segment_ids, row_start, row_count, 0)
        allowed = (key_pos[None, :] <= query_pos[:, None]) & (
            segment_ids[None, :key_count] == seg_query[:, None]
        )
        scores = jnp.where(allowed[None, None], scores, -1e30)
        row_max = jnp.max(scores, axis=-1, keepdims=True)
        raised = jnp.exp(scores - row_max)
        weights = (raised / jnp.sum(raised, axis=-1, keepdims=True)).astype(jnp.bfloat16)
        attended = jnp.einsum(
            "gpqk,kgd->qgpd", weights, kv_view[:, :, 1], preferred_element_type=jnp.float32
        )
        attended = attended.astype(jnp.bfloat16).reshape(row_count, q_heads * head_dim)
        projected = add_outputs(lax.all_gather(attended, "tp", axis=1, tiled=True))
        produced = (current.astype(jnp.float32) + projected).astype(jnp.bfloat16)
        done = step_idx - (pp_size - 1)
        if done >= 0:
            share = produced
            if done < pp_size - 1:
                share = lax.ppermute(produced, "pp", [(pp_size - 1, done)])
            hidden = jnp.where(section_idx == done, share, hidden)
        handed = shifted(produced, "pp", 1) if step_idx < step_count - 1 else produced
        return (handed, kv_buffer, hidden)

    initial = (
        jnp.zeros((row_count, local_width), jnp.bfloat16),
        jnp.zeros((row_total, held_heads * 2 * head_dim), jnp.bfloat16),
        jnp.zeros((row_count, local_width), jnp.bfloat16),
    )
    finished = initial
    for step_idx in range(step_count):
        finished = one_step(step_idx, finished)
    hidden = finished[2]
    kv_cache = own_pages(
        finished[1], page_rows, tp_rank, tensor_parallel_width, cache_page_count
    )
    return (hidden, kv_cache[None])


MESH = pl.DeviceIdType.MESH
LANES = 128
STREAM_CHUNKS = 4
MATMUL_ROWS = 128


def section_kernel(
    rows_of_mb,
    micro_batches,
    pp_size,
    tokens_hbm,
    gain_ref,
    wq_hbm,
    wkv_hbm,
    wo_hbm,
    table_ref,
    seg_row_ref,
    hidden_hbm,
    cache_hbm,
    wq,
    wkv,
    wo,
    stream,
    attended,
    keyval,
    gains,
    acc,
    proj,
    squares,
    landed,
    cache,
    seg_col,
    ids,
    wq_sem,
    wkv_sem,
    wo_sem,
    token_sem,
    gain_send,
    gain_recv,
    z_send,
    z_recv,
    y_send,
    y_recv,
    d_send,
    d_recv,
    r_send,
    r_recv,
    ay_send,
    ay_recv,
    ad_send,
    ad_recv,
    ar_send,
    ar_recv,
    k_send,
    k_recv,
    k_in,
    h_send,
    h_recv,
    out_sem,
    cache_sem,
):
    R, M, C = rows_of_mb, micro_batches, STREAM_CHUNKS
    width = stream.shape[2]
    model_width = 4 * width
    att_width = attended.shape[2]
    kv_width = keyval.shape[2]
    total_rows = stream.shape[1]
    q_width = wq.shape[1]
    chunk = width // C
    t = lax.axis_index("tp")
    sec = lax.axis_index("pp")
    last = pp_size - 1
    core = t % 2
    near = t + 1 - 2 * core
    far = (t + 2) % 4
    cross = (near + 2) % 4
    sources = (t, near, far, cross)
    score_scale = 1.0 / math.sqrt(HEAD_SIZE)
    per_section = M // pp_size

    def rows(i):
        return pl.ds(pl.multiple_of(i * R, R), R)

    def cols(c):
        return pl.ds(c * chunk, chunk)

    def remote(src, dst, send, recv, device):
        return pltpu.make_async_remote_copy(
            src_ref=src, dst_ref=dst, send_sem=send, recv_sem=recv, device_id=device, device_id_type=MESH
        )

    def wq_copy(s):
        k = pl.ds(pl.multiple_of(s * width, width), width)
        return pltpu.make_async_copy(wq_hbm.at[0, k], wq.at[k], wq_sem.at[s])

    def wkv_copy(s):
        k = pl.ds(pl.multiple_of(s * width, width), width)
        return pltpu.make_async_copy(wkv_hbm.at[0, k], wkv.at[k], wkv_sem.at[s])

    def wo_copy(s):
        a = pl.ds(pl.multiple_of(s * att_width, att_width), att_width)
        return pltpu.make_async_copy(wo_hbm.at[0, a], wo.at[a], wo_sem.at[s])

    def token_copy(i):
        return pltpu.make_async_copy(tokens_hbm.at[rows(i)], stream.at[t, rows(i)], token_sem.at[i])

    def y_copy(i, c):
        part = stream.at[t, rows(i), cols(c)]
        return remote(part, part, y_send.at[i], y_recv.at[i, c], {"tp": far})

    def d_copy(i, c):
        part = stream.at[t, rows(i), cols(c)]
        return remote(part, part, d_send.at[i], d_recv.at[i], {"tp": near})

    def r_copy(i, c):
        part = stream.at[far, rows(i), cols(c)]
        return remote(part, part, r_send.at[0], r_recv.at[i], {"tp": near})

    def z_copy(i, c):
        part = stream.at[t, rows(i), cols(c)]
        return remote(part, part, z_send.at[0], z_recv.at[i, c], {"pp": jnp.minimum(sec + 1, last)})

    def ay_copy(i):
        part = attended.at[t, rows(i)]
        return remote(part, part, ay_send.at[0], ay_recv.at[i], {"tp": far})

    def ad_copy(i):
        part = attended.at[t, rows(i)]
        return remote(part, part, ad_send.at[0], ad_recv.at[i], {"tp": near})

    def ar_copy(i):
        part = attended.at[far, rows(i)]
        return remote(part, part, ar_send.at[0], ar_recv.at[i], {"tp": near})

    def h_copy(i):
        return remote(
            stream.at[t, rows(i)],
            landed.at[rows(i % per_section)],
            h_send.at[0],
            h_recv.at[0],
            {"pp": i // per_section},
        )

    early_mbs = 3 * M // 4
    page_route = ((t, far), (t, near), (far, near))

    def k_copy(kind, i):
        which, to = page_route[kind]
        part = keyval.at[which, rows(i)]
        recv = k_recv.at[i] if kind == 0 else k_in.at[kind - 1, i // early_mbs]
        return remote(part, part, k_send.at[kind], recv, {"tp": to})

    def y_rows(i):
        part = stream.at[t, rows(i)]
        return remote(part, part, y_send.at[i], y_recv.at[i, 0], {"tp": far})

    def d_rows(i):
        part = stream.at[t, rows(i)]
        return remote(part, part, d_send.at[i], d_recv.at[i], {"tp": near})

    def r_rows(i):
        part = stream.at[far, rows(i)]
        return remote(part, part, r_send.at[0], r_recv.at[i], {"tp": near})

    def all_sent(part, send, recv):
        remote(part, part, send, recv, {"tp": near}).wait_send()

    def gain_copy(kind):
        return remote(gain_ref, gains.at[t], gain_send.at[kind], gain_recv.at[kind], {"tp": (near, far, cross)[kind]})

    @pl.when(sec == 0)
    def _():
        for i in range(M):
            token_copy(i).start()

    for s in sources:
        wq_copy(s).start()
        wkv_copy(s).start()
    for s in sources:
        wo_copy(s).start()

    barrier = pltpu.get_barrier_semaphore()
    for peer in (near, far, cross):
        pl.semaphore_signal(barrier, inc=1, device_id={"tp": peer}, device_id_type=MESH)
    for step in range(1, pp_size):
        pl.semaphore_signal(barrier, inc=1, device_id={"pp": (sec + step) % pp_size}, device_id_type=MESH)

    for n in range(total_rows // LANES):
        across = jnp.broadcast_to(seg_row_ref[:, n * LANES : (n + 1) * LANES].astype(jnp.float32), (LANES, LANES))
        seg_col[n * LANES : (n + 1) * LANES, :] = across.T
    heads, blocks = table_ref.shape[1:]
    spread = lax.broadcasted_iota(jnp.int32, (blocks, total_rows), 1) // PAGE_TOKENS
    spread = jnp.where(spread == lax.broadcasted_iota(jnp.int32, (blocks, total_rows), 0), 1.0, 0.0).astype(jnp.bfloat16)
    table = table_ref[0]
    upper = jnp.dot((table // 256).astype(jnp.float32).astype(jnp.bfloat16), spread, preferred_element_type=jnp.float32)
    lower = jnp.dot((table % 256).astype(jnp.float32).astype(jnp.bfloat16), spread, preferred_element_type=jnp.float32)
    in_page = lax.broadcasted_iota(jnp.int32, (heads, total_rows), 1) % PAGE_TOKENS
    ids[...] = (upper * 256.0 + lower) * PAGE_TOKENS + in_page.astype(jnp.float32)
    keyval[t] = jnp.zeros((total_rows, kv_width), jnp.bfloat16)
    gains[t] = gain_ref[...]
    pl.semaphore_wait(barrier, 3 + pp_size - 1)

    def forward(i, c):
        @pl.when(sec == 0)
        def _():
            if c == 0:
                token_copy(i).wait()

        @pl.when(sec > 0)
        def _():
            z_copy(i, c).wait_recv()

        y_copy(i, c).start()
        d_copy(i, c).start()

    def relay(i, c):
        y_copy(i, c).wait_recv()
        r_copy(i, c).start()

    def product(x, w):
        n = x.shape[0]
        if 2 * n <= MATMUL_ROWS:
            x = jnp.concatenate([x, x], axis=0)
        return jnp.dot(x, w, preferred_element_type=jnp.float32)[:n]

    def take(i, s):
        x = stream[s, rows(i)]
        wide = x.astype(jnp.float32)
        sq = wide * wide
        part = sq[:, :LANES]
        for j in range(1, width // LANES):
            part = part + sq[:, j * LANES : (j + 1) * LANES]
        y = x * gains[s]
        k = pl.ds(pl.multiple_of(s * width, width), width)
        return part, product(y, wq[k, :]), product(y, wkv[k, :])

    def near_part(i):
        a, b = take(i, t), take(i, near)
        squares[...] = a[0] + b[0]
        acc[:, :q_width] = a[1] + b[1]
        acc[:, q_width:] = a[2] + b[2]

    def far_part(i):
        a = take(i, far)
        squares[...] += a[0]
        acc[:, :q_width] += a[1]
        acc[:, q_width:] += a[2]

    def attend(i):
        a = take(i, cross)
        mean_sq = jnp.sum(squares[...] + a[0], axis=1, keepdims=True) / model_width
        scale = lax.rsqrt(mean_sq + eps_norm)
        q = ((acc[:, :q_width] + a[1]) * scale).astype(jnp.bfloat16)
        keyval[t, rows(i)] = ((acc[:, q_width:] + a[2]) * scale).astype(jnp.bfloat16)
        q_pos = i * R + lax.broadcasted_iota(jnp.int32, (R, total_rows), 0)
        k_pos = lax.broadcasted_iota(jnp.int32, (R, total_rows), 1)
        same = seg_row_ref[...].astype(jnp.float32) == seg_col[rows(i), 0:1]
        bias = jnp.where((k_pos <= q_pos) & same, 0.0, -1e30).astype(jnp.float32)
        held = kv_width // (2 * HEAD_SIZE)
        per_kv = q_width // HEAD_SIZE // held
        for g in range(held):
            at = g * 2 * HEAD_SIZE
            keys = keyval[t, :, at : at + HEAD_SIZE]
            values = keyval[t, :, at + HEAD_SIZE : at + 2 * HEAD_SIZE]
            heads = range(g * per_kv, (g + 1) * per_kv)
            qg = jnp.concatenate([q[:, j * HEAD_SIZE : (j + 1) * HEAD_SIZE] for j in heads], axis=0)
            s = lax.dot_general(qg, keys, (((1,), (1,)), ((), ())), preferred_element_type=jnp.float32)
            s = s.reshape(per_kv, R, total_rows) * score_scale + bias[None]
            s = s.reshape(per_kv * R, total_rows)
            raised = jnp.exp(s - jnp.max(s, axis=-1, keepdims=True))
            mass = jnp.sum(raised, axis=-1, keepdims=True)
            mixed = jnp.dot(raised.astype(jnp.bfloat16), values, preferred_element_type=jnp.float32) / mass
            mixed = mixed.astype(jnp.bfloat16)
            for n, j in enumerate(heads):
                attended[t, rows(i), j * HEAD_SIZE : (j + 1) * HEAD_SIZE] = mixed[n * R : (n + 1) * R]
        ay_copy(i).start()
        ad_copy(i).start()

        @pl.when(sec == last)
        def _():
            k_copy(0, i).start()
            k_copy(1, i).start()

    def out_rows(s):
        return pl.ds(pl.multiple_of(s * att_width, att_width), att_width)

    def from_att(i, s, at):
        return product(attended[s, rows(i)], wo[out_rows(s), at])

    def near_out(i):
        ad_copy(i).wait_recv()
        every = slice(None)
        proj[...] = from_att(i, t, every) + from_att(i, near, every)

    def relay_att(i):
        ay_copy(i).wait_recv()
        ar_copy(i).start()

    def far_out(i):
        y_rows(i).wait_send()
        d_rows(i).wait_send()
        ar_copy(i).wait_recv()
        wide = 2 * chunk
        for n in range(C // 2):
            at = pl.ds(n * wide, wide)
            add = from_att(i, far, at) + from_att(i, cross, at)
            whole = stream[t, rows(i), at].astype(jnp.float32) + (proj[:, at] + add)
            stream[t, rows(i), at] = whole.astype(jnp.bfloat16)

            @pl.when(sec < last)
            def _():
                z_copy(i, 2 * n).start()
                z_copy(i, 2 * n + 1).start()

        @pl.when((sec == last) & (i // per_section < last))
        def _():
            h_copy(i).start()

    cache_rows = cache.shape[0]
    block = cache_rows // 4
    held = kv_width // (2 * HEAD_SIZE)
    def cache_store(b):
        at = pl.ds(pl.multiple_of(b * block, block), block)
        return pltpu.make_async_copy(cache.at[at], cache_hbm.at[at], cache_sem.at[0])

    def assemble(lo, hi, final_part):
        at = slice(lo * R, hi * R)

        def one_block(b, carry):
            start = pl.multiple_of(b * block, block)
            row = lax.broadcasted_iota(jnp.int32, (block, (hi - lo) * R), 0)
            row = (row + t * cache_rows + start).astype(jnp.float32)
            total = jnp.zeros((block, 2 * HEAD_SIZE), jnp.float32)
            for s in range(4):
                for g in range(held):
                    head = s * held + g
                    onehot = jnp.where(ids[head : head + 1, at] == row, 1.0, 0.0).astype(jnp.bfloat16)
                    pages = keyval[s, at, g * 2 * HEAD_SIZE : (g + 1) * 2 * HEAD_SIZE]
                    total = total + jnp.dot(onehot, pages, preferred_element_type=jnp.float32)
            if final_part:
                total = total + cache[pl.ds(start, block), :].astype(jnp.float32)
            cache[pl.ds(start, block), :] = total.astype(jnp.bfloat16)
            if final_part:
                cache_store(b).start()
            return carry

        lax.fori_loop(0, 4, one_block, 0)

    def relay_pages(i):
        k_copy(0, i).wait_recv()
        k_copy(2, i).start()

    def pages_in(lo, hi):
        for kind in (1, 2):
            which, to = page_route[kind]
            part = keyval.at[which, pl.ds(lo * R, (hi - lo) * R)]
            remote(part, part, k_send.at[kind], k_in.at[kind - 1, lo // early_mbs], {"tp": to}).wait_recv()

    for kind in range(3):
        gain_copy(kind).start()
    for c in range(C):
        forward(0, c)
    wq_copy(t).wait()
    wkv_copy(t).wait()
    wq_copy(near).wait()
    wkv_copy(near).wait()
    for kind in range(3):
        gain_copy(kind).wait_recv()
    d_rows(0).wait_recv()
    near_part(0)
    for c in range(C):
        relay(0, c)
    first, final = sec == 0, sec == last
    middle = (sec > 0) & (sec < last)

    @pl.when(first | final)
    def _():
        for c in range(C // 2):
            forward(1, c)

    wq_copy(far).wait()
    wkv_copy(far).wait()
    far_part(0)
    wq_copy(cross).wait()
    wkv_copy(cross).wait()

    @pl.when(middle)
    def _():
        for c in range(C // 2):
            forward(1, c)

    for c in range(C // 2, C):
        forward(1, c)
    r_rows(0).wait_recv()
    attend(0)
    for s in sources:
        wo_copy(s).wait()

    def one(i, carry):
        def ahead(where, *chunks):
            @pl.when((i + 2 < M) & where)
            def _():
                for c in chunks:
                    forward(i + 2, c)

        d_rows(i + 1).wait_recv()
        near_part(i + 1)
        ahead(first, 0, 1)
        ahead(sec > 0, 0)
        near_out(i)
        ahead(middle, 1)
        ahead(final, 1, 2)
        for c in range(C):
            relay(i + 1, c)
        far_part(i + 1)
        ahead(sec < last, 2)
        ahead(final, 3)
        relay_att(i)
        ahead(first, 3)
        r_rows(i + 1).wait_recv()
        attend(i + 1)
        ahead(middle, 3)

        @pl.when(sec == last)
        def _():
            relay_pages(i)

        far_out(i)
        return carry

    lax.fori_loop(0, M - 1, one, 0)
    near_out(M - 1)

    @pl.when(sec == last)
    def _():
        pages_in(0, early_mbs)
        assemble(0, early_mbs, False)

    relay_att(M - 1)

    @pl.when(sec == last)
    def _():
        relay_pages(M - 1)

    far_out(M - 1)

    @pl.when(sec < last)
    def _():
        def send_pages(i, carry):
            k_copy(0, i).start()
            k_copy(1, i).start()
            return carry

        def pass_pages(i, carry):
            relay_pages(i)
            return carry

        lax.fori_loop(0, M, send_pages, 0)
        lax.fori_loop(0, M, pass_pages, 0)
        pages_in(0, early_mbs)
        assemble(0, early_mbs, False)
        remote(landed, landed, h_send.at[0], h_recv.at[0], {"pp": 0}).wait_recv()
        done = pltpu.make_async_copy(landed, hidden_hbm, out_sem.at[0])
        done.start()
        done.wait()

    mine = stream.at[t, pl.ds((M - per_section) * R, per_section * R)]

    @pl.when(sec == last)
    def _():
        pltpu.make_async_copy(mine, hidden_hbm, out_sem.at[0]).start()

    pages_in(early_mbs, M)
    assemble(early_mbs, M, True)

    all_sent(stream.at[far], r_send.at[0], r_recv.at[0])
    all_sent(attended.at[t], ay_send.at[0], ay_recv.at[0])
    all_sent(attended.at[t], ad_send.at[0], ad_recv.at[0])
    all_sent(attended.at[far], ar_send.at[0], ar_recv.at[0])
    for kind in range(3):
        all_sent(keyval.at[page_route[kind][0]], k_send.at[kind], k_recv.at[0])

    @pl.when(sec < last)
    def _():
        all_sent(stream.at[t], z_send.at[0], z_recv.at[0, 0])

    @pl.when(sec == last)
    def _():
        all_sent(stream.at[t, pl.ds(0, (M - per_section) * R)], h_send.at[0], h_recv.at[0])

    for kind in range(3):
        gain_copy(kind).wait_send()

    @pl.when(sec == last)
    def _():
        pltpu.make_async_copy(mine, hidden_hbm, out_sem.at[0]).wait()

    pltpu.make_async_copy(cache, cache_hbm, cache_sem.at[0]).wait()


def kernel_body(tokens, gain, q_weight, kv_weight, out_weight, page_table, segment_ids):
    pp_size = lax.axis_size("pp")
    total_rows, width = tokens.shape
    M = 2 * pp_size
    R = total_rows // M
    q_width, kv_width = q_weight.shape[2], kv_weight.shape[2]
    att_all = out_weight.shape[1]
    att_width = att_all // 4
    heads = page_table.shape[1]
    cache_rows = heads * total_rows // 4
    any_spec = pl.BlockSpec(memory_space=pl.ANY)
    vmem_spec = pl.BlockSpec(memory_space=pltpu.VMEM)
    dma = pltpu.SemaphoreType.DMA
    C = STREAM_CHUNKS
    bf16, f32 = jnp.bfloat16, jnp.float32
    hidden, cache = pl.pallas_call(
        functools.partial(section_kernel, R, M, pp_size),
        out_shape=(
            jax.ShapeDtypeStruct((total_rows // pp_size, width), bf16),
            jax.ShapeDtypeStruct((cache_rows, 2 * HEAD_SIZE), bf16),
        ),
        in_specs=[any_spec, vmem_spec, any_spec, any_spec, any_spec, vmem_spec, vmem_spec],
        out_specs=(any_spec, any_spec),
        scratch_shapes=[
            pltpu.VMEM((4 * width, q_width), bf16),
            pltpu.VMEM((4 * width, kv_width), bf16),
            pltpu.VMEM((att_all, width), bf16),
            pltpu.VMEM((4, total_rows, width), bf16),
            pltpu.VMEM((4, total_rows, att_width), bf16),
            pltpu.VMEM((4, total_rows, kv_width), bf16),
            pltpu.VMEM((4, 1, width), bf16),
            pltpu.VMEM((R, q_width + kv_width), f32),
            pltpu.VMEM((R, width), f32),
            pltpu.VMEM((R, LANES), f32),
            pltpu.VMEM((total_rows // pp_size, width), bf16),
            pltpu.VMEM((cache_rows, 2 * HEAD_SIZE), bf16),
            pltpu.VMEM((total_rows, LANES), f32),
            pltpu.VMEM((heads, total_rows), f32),
            dma((4,)),
            dma((4,)),
            dma((4,)),
            dma((M,)),
            dma((3,)),
            dma((3,)),
            dma((1,)),
            dma((M, C)),
            dma((M,)),
            dma((M, C)),
            dma((M,)),
            dma((M,)),
            dma((1,)),
            dma((M,)),
            dma((1,)),
            dma((M,)),
            dma((1,)),
            dma((M,)),
            dma((1,)),
            dma((M,)),
            dma((3,)),
            dma((M,)),
            dma((2, 2)),
            dma((1,)),
            dma((1,)),
            dma((1,)),
            dma((1,)),
        ],
        compiler_params=pltpu.CompilerParams(
            collective_id=0, has_side_effects=True, vmem_limit_bytes=67043328
        ),
    )(
        tokens,
        gain,
        q_weight,
        kv_weight,
        out_weight,
        page_table,
        segment_ids[None, :],
    )
    pages = cache.reshape(1, cache_rows // PAGE_TOKENS, PAGE_TOKENS, 2 * HEAD_SIZE)
    return hidden, pages


def chosen_body(tokens, gain, q_weight, kv_weight, out_weight, page_table, segment_ids):
    whole_heads = kv_weight.shape[2] % (2 * HEAD_SIZE) == 0
    rows_fit = tokens.shape[0] % (32 * lax.axis_size("pp")) == 0
    if lax.axis_size("tp") == 4 and whole_heads and rows_fit:
        return kernel_body(tokens, gain, q_weight, kv_weight, out_weight, page_table, segment_ids)
    return body(tokens, gain, q_weight, kv_weight, out_weight, page_table, segment_ids)


def solution(mesh):
    placed = (
        P("grp", "tp"),
        P("pp", "tp"),
        P("pp", None, "tp"),
        P("pp", None, "tp"),
        P("pp", None, "tp"),
        P("pp", None, None),
        P("grp"),
    )
    return jax.shard_map(
        chosen_body,
        mesh=mesh,
        in_specs=placed,
        out_specs=(P(("grp", "pp"), "tp"), P("pp", ("grp", "tp"), None, None)),
        check_vma=False,
    )
```
